512 devices in a mesh: gx: 16 (over z), gy: 8 (over y, core), gz: 4 (over x).
Axes of the slice: x: 4, y: 4, z: 16, core: 2. Of those that a mesh axis runs over, the one named last changes fastest.
Arguments:
- nodal_warmth_degrees: float32 [3, 3, 3, 64, 32, 512], P(None, None, None, 'gx', 'gy', 'gz'), may hold values from -6 to 6
- thermal_transfer_coefficient: float32 [64, 32, 512], P('gx', 'gy', 'gz'), may hold values from 0.1 to 2
- taken_beam_fraction: float32 [64, 32, 512], P('gx', 'gy', 'gz'), may hold values from 0.3 to 3
- laid_tiers: int32 [16, 8, 4], P('gx', 'gy', 'gz'), may hold values from 64 to 128
- holding_brick_column: int32 [16, 8, 4, 2048, 1], P('gx', 'gy', 'gz'), may hold values from 0 to 15; in each aligned block of 2048 rows (0 to 2047, 2048 to 4095, ..., all dimensions but the last counted through in order) at most 256 rows name the same one
- piece_onto_solid_brick: int32 [16, 8, 4, 2048], P('gx', 'gy', 'gz'), may hold values from 0 to 255, as said below
- deformation_change: float32 [6, 8, 131072], P(None, None, ('gx', 'gy', 'gz')), may hold values from -0.06 to 0.06
- earlier_tension_state: float32 [6, 8, 131072], P(None, None, ('gx', 'gy', 'gz')), may hold values from -3 to 3
- plastic_onset_threshold: float32 [131072], P(('gx', 'gy', 'gz')), may hold values from 0.5 to 2
Outputs:
- temperature_new: float32 [3, 3, 3, 64, 32, 512], P(None, None, None, 'gx', 'gy', 'gz')
- stress_new: float32 [6, 8, 131072], P(None, None, ('gx', 'gy', 'gz'))
- forces: float32 [3, 8, 131072], P(None, None, ('gx', 'gy', 'gz'))
The draws below stay inside these ranges and needn't reach their ends.
Inputs may be any that keep to these rules, and one draw needn't show every extreme that they name: `holding_brick_column`: the elements of one device hand at most 256 elements to one owner; in every draw some device hands exactly 256 to some owner. `piece_onto_solid_brick`: some mechanical cells may receive no element.
All inputs are finite; a program needn't handle non-finite values.
Results may differ from the reference program's by a relative error of at most 0.00022.
Values sent between devices are 32-bit elements; how exact they have to be, the bound alone decides.
No kernel may reach another device: no remote copies, remote signals or barrier semaphores. Data moves between devices by JAX's collectives and lax.ppermute only.
A program may use at most 64 MiB of HBM per device.

```python
import math
import jax
import jax.numpy as jnp
import numpy as np
from jax import lax

PART_PIECES_LONG = 4
PART_PIECES_WIDE = 4
PART_PIECES_TALL = 128
STEPS = 4
PLATE_PIECES_LONG = 64
PLATE_PIECES_WIDE = 32
PLATE_PIECES_TALL = 512
ELEM_DEV = 2048
CAP = 256
MC_DEV = 256
MC_TOTAL = 131072
N_GX = 16
N_GY = 8
N_GZ = 4


def draw_piece_onto_solid_brick(key, part):
    empty_cell = jax.random.randint(jax.random.fold_in(key, 11), (1, N_GY, N_GZ, 1), 0, MC_DEV)
    drawn = jax.random.randint(jax.random.fold_in(key, 12), (N_GX, N_GY, N_GZ, ELEM_DEV), 0, MC_DEV - 1)
    return (drawn + (drawn >= empty_cell).astype(jnp.int32)).astype(jnp.int32)


def plant(result, stream_key, smallest, top_value):
    spot = [jax.random.randint(jax.random.fold_in(stream_key, axis), (), 0, length) for axis, length in enumerate(result.shape)]
    longest = result.shape.index(max(result.shape))
    neighbour = spot[:longest] + [(spot[longest] + 1) % result.shape[longest]] + spot[longest + 1:]
    return result.at[tuple(spot)].set(smallest).at[tuple(neighbour)].set(top_value)


def levels(own_key, shape, shards, least, high):
    level = 1.0
    for position, blocks in shards:
        draws = jax.random.uniform(jax.random.fold_in(jax.random.fold_in(own_key, 6), position), (blocks,), jnp.float32, least / len(shards), high / len(shards))
        level = level * jnp.repeat(jnp.exp(draws), shape[position] // blocks).reshape((-1,) + (1,) * (len(shape) - 1 - position))
    return level


def deal_out(stream_key, own, number, rows, number_of, top, most, lean):
    order = jax.random.permutation(stream_key, number_of)
    packed, ordinary = load_shares(number_of, rows * top, most, lean, True), load_shares(number_of, rows * top, most, lean, False)
    places = jnp.arange(number_of)

    def named(lengths, rotation):
        used = int((lengths > 0).sum())
        fixed = max(1, used // 4)
        shifted = fixed + (places - fixed + rotation * (used - fixed)) % max(1, number_of - fixed)
        return jnp.zeros((number_of,), jnp.int32).at[order[jnp.where(places < fixed, places, shifted)]].set(jnp.asarray(lengths, jnp.int32))

    lengths = jnp.where(number % 4 == 0, named(packed, number // 4), named(ordinary, number - number // 4 - 1))
    mixed = jax.random.permutation(jax.random.fold_in(own, 3), number_of)
    donor, sink = mixed[0:number_of // 2 * 2:2], mixed[1:number_of // 2 * 2:2]
    margin = jnp.minimum(lengths[donor] - 1, most - lengths[sink]) // 2
    margin = jnp.where((donor == order[0]) | (sink == order[0]) | (lengths[sink] == 0), 0, jnp.maximum(margin, 0))
    shifted = jax.random.randint(jax.random.fold_in(own, 4), (number_of // 2,), 0, 1 << 20) % (margin + 1)
    lengths = lengths.at[donor].add(-shifted).at[sink].add(shifted)
    items = jnp.searchsorted(jnp.cumsum(lengths), jnp.arange(rows * top), side="right").astype(jnp.int32)
    table = items.reshape(top, rows).T
    table = table[jax.random.permutation(jax.random.fold_in(own, 1), rows)]
    rotation = jax.random.randint(jax.random.fold_in(own, 2), (rows, 1), 0, top)
    return jnp.take_along_axis(table, (jnp.arange(top)[None, :] + rotation) % top, axis=1)


def load_shares(number_of, total, bound, skew, full):
    loads = [(1 << 20) // math.isqrt(grade ** skew) + 1 for grade in range(1, number_of + 1)]
    largest = bound if full else min(bound, max(-(-total // number_of), total * loads[0] // sum(loads)))
    least = 1 if total - largest >= number_of - 1 else 0
    given, spare = [largest] + [least] * (number_of - 1), total - largest - least * (number_of - 1)
    while spare > 0:
        movable = [i for i in range(1, number_of) if given[i] < largest] or [i for i in range(1, number_of) if given[i] < bound]
        pool, remaining = sum([loads[i] for i in movable]), spare
        for i in movable:
            more = min(bound - given[i], max(1, remaining * loads[i] // pool), spare)
            given[i] = given[i] + more
            spare = spare - more
    return np.array(given)


def normal_values(rng, dims, scale, bound, split=(), held_as=jnp.bfloat16):
    entries = jax.random.normal(rng, dims, jnp.float32) * scale
    if len(split) > 0:
        entries = levels(rng, dims, split, -0.22, 0.18) * entries
    return jnp.clip(entries, min=-bound, max=bound).astype(held_as)


def setup_inputs(seed: int = 0) -> dict:
    key_of = jax.random.split(jax.random.key(seed), 10)
    nodal_warmth_degrees = normal_values(key_of[0], (3, 3, 3, PLATE_PIECES_LONG, PLATE_PIECES_WIDE, PLATE_PIECES_TALL), 1.0, 6.0, ((3, 16), (4, 8), (5, 4)), jnp.float32)
    thermal_transfer_coefficient = jnp.clip(jnp.exp(math.log(2.0) - 2.9957323 * jax.random.uniform(key_of[1], (PLATE_PIECES_LONG, PLATE_PIECES_WIDE, PLATE_PIECES_TALL), jnp.float32) ** levels(key_of[1], (PLATE_PIECES_LONG, PLATE_PIECES_WIDE, PLATE_PIECES_TALL), ((0, 16), (1, 8), (2, 4)), -0.2, 0.2)), 0.1, 2.0)
    taken_beam_fraction = jnp.clip(jnp.exp(math.log(3.0) - 2.3025851 * jax.random.uniform(key_of[2], (PLATE_PIECES_LONG, PLATE_PIECES_WIDE, PLATE_PIECES_TALL), jnp.float32) ** levels(key_of[2], (PLATE_PIECES_LONG, PLATE_PIECES_WIDE, PLATE_PIECES_TALL), ((0, 16), (1, 8), (2, 4)), -0.2, 0.2)), 0.3, 3.0)
    laid_tiers = plant(jax.random.randint(key_of[3], (N_GX, N_GY, N_GZ), PART_PIECES_TALL // 2, PART_PIECES_TALL + 1), jax.random.fold_in(key_of[3], 1), PART_PIECES_TALL // 2, PART_PIECES_TALL).astype(jnp.int32)
    holding_brick_column_keys = jax.random.split(jax.random.fold_in(key_of[4], 1), N_GX * N_GY * N_GZ * ELEM_DEV // ELEM_DEV)
    holding_brick_column_turns = jax.random.permutation(jax.random.fold_in(key_of[4], 3), N_GX * N_GY * N_GZ * ELEM_DEV // ELEM_DEV)
    holding_brick_column = jax.vmap(lambda own, number: deal_out(jax.random.fold_in(key_of[4], 2), own, number, ELEM_DEV, N_GX, 1, CAP, 2))(holding_brick_column_keys, holding_brick_column_turns).reshape((N_GX, N_GY, N_GZ, ELEM_DEV, 1))
    piece_onto_solid_brick = draw_piece_onto_solid_brick(jax.random.fold_in(key_of[9], 71), 0)
    deformation_change = normal_values(key_of[6], (6, 8, MC_TOTAL), 0.01, 0.06, ((2, 512),), jnp.float32)
    earlier_tension_state = normal_values(key_of[7], (6, 8, MC_TOTAL), 0.5, 3.0, ((2, 512),), jnp.float32)
    plastic_onset_threshold = jnp.clip(jnp.exp(math.log(2.0) - 1.3862944 * jax.random.uniform(key_of[8], (MC_TOTAL,), jnp.float32) ** levels(key_of[8], (MC_TOTAL,), ((0, 512),), -0.2, 0.2)), 0.5, 2.0)
    return dict(nodal_warmth_degrees=nodal_warmth_degrees, thermal_transfer_coefficient=thermal_transfer_coefficient, taken_beam_fraction=taken_beam_fraction, laid_tiers=laid_tiers, holding_brick_column=holding_brick_column, piece_onto_solid_brick=piece_onto_solid_brick, deformation_change=deformation_change, earlier_tension_state=earlier_tension_state, plastic_onset_threshold=plastic_onset_threshold)


time_step = 0.003
penalty = 3.0
heat_power = 100.0
expansion = 0.02
shear_modulus = 100.0 / 2.6
lame_first = 30.0 / 0.52
hardening = 10.0
highest = lax.Precision.HIGHEST
nodal_weights = np.array([1.0 / 6.0, 2.0 / 3.0, 1.0 / 6.0], np.float32)

def lumped_line():
    stiff = np.array([[7.0, -8.0, 1.0], [-8.0, 16.0, -8.0], [1.0, -8.0, 7.0]], np.float32) / 3.0
    return stiff / nodal_weights[:, None]

def gauss_spots():
    half = 0.5 / math.sqrt(3.0)
    return [0.5 - half, 0.5 + half]

def gauss_values():
    rows = []
    for point in gauss_spots():
        rows.append([2.0 * (point - 0.5) * (point - 1.0), -4.0 * point * (point - 1.0), 2.0 * point * (point - 0.5)])
    return np.array(rows, np.float32)

def gradient_table():
    spots = gauss_spots()
    table = np.zeros((3, 8, 8), np.float32)
    for node in range(8):
        corner = [node // 4, node // 2 % 2, node % 2]
        for point in range(8):
            place = [spots[point // 4], spots[point // 2 % 2], spots[point % 2]]
            values = [place[k] if corner[k] else 1.0 - place[k] for k in range(3)]
            slopes = [1.0 if corner[k] else -1.0 for k in range(3)]
            table[0, node, point] = slopes[0] * values[1] * values[2] / 8.0
            table[1, node, point] = values[0] * slopes[1] * values[2] / 8.0
            table[2, node, point] = values[0] * values[1] * slopes[2] / 8.0
    return table

def window(array, lead, axis, offset):
    index = [slice(None)] * lead
    for k in range(3):
        move = offset if k == axis else 0
        index.append(slice(1 + move, array.shape[lead + k] - 1 + move))
    return array[tuple(index)]

def node_terms(anchor, count, centre, near, far):
    places = (jnp.arange(count) + anchor).astype(jnp.float32)[None, :] + 0.5 * jnp.arange(3).astype(jnp.float32)[:, None]
    offset = places - centre
    radius = jnp.where(offset >= 0.0, near, far)
    return -3.0 * (offset / radius) ** 2

def advance_solution(nodal_quantity_entries, diffusivity, mask, absorb_heat, anchor, step_forward, extent):
    core = window(nodal_quantity_entries, 3, 0, 0)
    kcore = window(diffusivity, 0, 0, 0)
    mcore = window(mask, 0, 0, 0)
    acore = window(absorb_heat, 0, 0, 0)
    line = jnp.asarray(lumped_line())
    rate = jnp.einsum('ai,ibcxyz->abcxyz', line, core, precision=highest)
    rate = rate + jnp.einsum('bi,aicxyz->abcxyz', line, core, precision=highest)
    rate = rate + jnp.einsum('ci,abixyz->abcxyz', line, core, precision=highest)
    rate = -kcore * rate
    for axis in range(3):
        for offset, own, other in ((1, 2, 0), (-1, 0, 2)):
            beside = window(nodal_quantity_entries, 3, axis, offset)
            kbeside = window(diffusivity, 0, axis, offset)
            mbeside = window(mask, 0, axis, offset)
            couple = penalty * 2.0 * kcore * kbeside / jnp.maximum(kcore + kbeside, 1.0) * mcore * mbeside
            jump = jnp.take(core, own, axis=axis) - jnp.take(beside, other, axis=axis)
            flux = couple * jump / float(nodal_weights[own])
            rate = rate.at[(slice(None),) * axis + (own,)].add(-flux)
    length, width, height = extent
    shape = core.shape
    xterm = node_terms(anchor[0], shape[3], length * 0.5 + step_forward * length / 16.0, length / 8.0, length / 4.0)
    yterm = node_terms(anchor[1], shape[4], width * 0.5, width / 4.0, width / 4.0)
    zterm = node_terms(anchor[2], shape[5], height * 0.75, height / 8.0, height / 8.0)
    total = xterm[:, None, None, :, None, None] + yterm[None, :, None, None, :, None] + zterm[None, None, :, None, None, :]
    source = heat_power * (2.0 / 3.0) * jnp.exp(total) * acore
    return core + time_step * mcore * (rate + source)

def gauss_point_change(change):
    table = jnp.asarray(gauss_values())
    value = jnp.einsum('pa,abcxyz->pbcxyz', table, change, precision=highest)
    value = jnp.einsum('qb,pbcxyz->pqcxyz', table, value, precision=highest)
    value = jnp.einsum('rc,pqcxyz->pqrxyz', table, value, precision=highest)
    return value

def mechanics(deformation_change, earlier_tension_state, plastic_onset_threshold, thermal):
    normal_component = deformation_change[0:3] - expansion * thermal[None]
    volume = normal_component[0] + normal_component[1] + normal_component[2]
    trial_normal = earlier_tension_state[0:3] + lame_first * volume[None] + 2.0 * shear_modulus * normal_component
    trial_shear = earlier_tension_state[3:6] + 2.0 * shear_modulus * deformation_change[3:6]
    pressure = (trial_normal[0] + trial_normal[1] + trial_normal[2]) / 3.0
    dev_normal = trial_normal - pressure[None]
    squares = lax.optimization_barrier(jnp.sum(dev_normal * dev_normal, axis=0)) + 2.0 * lax.optimization_barrier(jnp.sum(trial_shear * trial_shear, axis=0))
    equivalent = jnp.sqrt(1.5 * squares)
    limit = plastic_onset_threshold[None, :]
    plastic = jnp.maximum(equivalent - limit, 0.0) / (3.0 * shear_modulus + hardening)
    factor = 1.0 - 3.0 * shear_modulus * plastic / jnp.maximum(equivalent, limit)
    new_normal = pressure[None] + factor[None] * dev_normal
    new_shear = factor[None] * trial_shear
    stress_new = jnp.concatenate([new_normal, new_shear], axis=0)
    rows = [[0, 5, 4], [5, 1, 3], [4, 3, 2]]
    tensor = jnp.stack([jnp.stack([stress_new[k] for k in row], axis=0) for row in rows], axis=0)
    forces = jnp.einsum('dig,cdgm->cim', jnp.asarray(gradient_table()), tensor, precision=highest)
    return (stress_new, forces)

def reference(nodal_warmth_degrees, thermal_transfer_coefficient, taken_beam_fraction, laid_tiers, holding_brick_column, piece_onto_solid_brick, deformation_change, earlier_tension_state, plastic_onset_threshold):
    full_layers = jnp.repeat(jnp.repeat(jnp.repeat(laid_tiers, PART_PIECES_LONG, axis=0), PART_PIECES_WIDE, axis=1), PART_PIECES_TALL, axis=2)
    device_height = jnp.arange(PLATE_PIECES_TALL) % PART_PIECES_TALL
    mask = (device_height[None, None, :] < full_layers).astype(jnp.float32)

    def cycle_index(array, lead):
        return jnp.pad(array, [(0, 0)] * lead + [(1, 1)] * 3)
    diffusivity = cycle_index(thermal_transfer_coefficient, 0)
    masked_values = cycle_index(mask, 0)
    absorb_heat = cycle_index(taken_beam_fraction, 0)
    nodal_quantity_entries = nodal_warmth_degrees
    for step_forward in range(STEPS):
        nodal_quantity_entries = advance_solution(cycle_index(nodal_quantity_entries, 3), diffusivity, masked_values, absorb_heat, (0, 0, 0), step_forward, (PLATE_PIECES_LONG, PLATE_PIECES_WIDE, PLATE_PIECES_TALL))
    change_amount_entry = gauss_point_change(nodal_quantity_entries - nodal_warmth_degrees).reshape(8, N_GX, PART_PIECES_LONG, N_GY, PART_PIECES_WIDE, N_GZ, PART_PIECES_TALL)
    change_amount_entry = jnp.transpose(change_amount_entry, (0, 1, 3, 5, 2, 4, 6)).reshape(8, -1)
    weights = jnp.transpose(mask.reshape(N_GX, PART_PIECES_LONG, N_GY, PART_PIECES_WIDE, N_GZ, PART_PIECES_TALL), (0, 2, 4, 1, 3, 5)).reshape(-1)
    row_y = jnp.arange(N_GY).astype(jnp.int32)[None, :, None, None]
    row_z = jnp.arange(N_GZ).astype(jnp.int32)[None, None, :, None]
    target = ((holding_brick_column[..., 0] * N_GY + row_y) * N_GZ + row_z) * MC_DEV + piece_onto_solid_brick
    target = target.reshape(-1).astype(jnp.int32)
    sums = jnp.zeros((8, MC_TOTAL), jnp.float32).at[:, target].add(change_amount_entry * weights[None, :])
    counts = jnp.zeros((MC_TOTAL,), jnp.float32).at[target].add(weights)
    thermal = sums / jnp.maximum(counts, 1.0)[None, :]
    stress_new, forces = mechanics(deformation_change, earlier_tension_state, plastic_onset_threshold, thermal)
    return (nodal_quantity_entries, stress_new, forces)
```

```python
import functools
import math

import jax
import jax.numpy as jnp
import numpy as np
from jax import lax
from jax.experimental import pallas as pl
from jax.experimental.pallas import tpu as pltpu
from jax.sharding import PartitionSpec as P

STEPS = 4
DT = 0.003
PENALTY = 3.0
HEAT = 100.0 * (2.0 / 3.0)
EXPANSION = 0.02
MU = 100.0 / 2.6
LAME = 30.0 / 0.52
HARD = 10.0
NX, NY, NZ = 64, 32, 512
PX, PY, PZ = 4, 4, 128
OWNERS, CELLS = 16, 256
F32 = jnp.float32

LAM = (0.0, 12.0, 24.0)
XROWS = 480
YROWS = 928
CORNERS = [(side, xd, d) for side in (0, 1) for xd in (1, 2, 3) for d in range(1, 5 - xd)]


def mode(i, j, l):
    return 9 * i + 3 * j + l


def call(kernel, outs, args, scratch=(), smem=(), near=()):
    args = [
        pltpu.with_memory_space_constraint(a, pltpu.VMEM) if n in near else a
        for n, a in enumerate(args)
    ]
    specs = [
        pl.BlockSpec(memory_space=pltpu.SMEM if n in smem else pltpu.VMEM) for n in range(len(args))
    ]
    return pl.pallas_call(
        kernel,
        out_shape=outs,
        in_specs=specs,
        out_specs=jax.tree.map(lambda _: pl.BlockSpec(memory_space=pltpu.VMEM), outs),
        scratch_shapes=list(scratch),
    )(*args)


def lane_iota(rows):
    return lax.broadcasted_iota(jnp.int32, (rows, 128), 1)


def row_iota(rows):
    return lax.broadcasted_iota(jnp.int32, (rows, 128), 0)


def modal(a, b, c):
    s = a + c
    return (s + 4.0 * b) * (1.0 / 6.0), (c - a) * 0.5, (s - 2.0 * b) * (1.0 / 3.0)


def modal_grid(values):
    for stride in (9, 3, 1):
        out = [None] * 27
        for base in range(27):
            if base // stride % 3 == 0:
                ids = [base + stride * t for t in range(3)]
                for q, r in zip(ids, modal(*[values[q] for q in ids])):
                    out[q] = r
        values = out
    return values


def nodal_grid(values):
    for stride in (9, 3, 1):
        out = [None] * 27
        for base in range(27):
            if base // stride % 3 == 0:
                al, be, ga = (values[base + stride * t] for t in range(3))
                e = al + ga
                out[base], out[base + stride], out[base + 2 * stride] = e - be, al - 0.5 * ga, e + be
        values = out
    return values


def prep_kernel(t_ref, k_ref, a_ref, lay_ref, cols_ref, zpay_ref):
    layers = lay_ref[0]
    m = (lane_iota(8) < layers).astype(F32)
    lane = lane_iota(32)
    for h in range(2):
        rows = slice(8 * h, 8 * h + 8)
        modes = modal_grid([t_ref[n, rows, :] for n in range(27)])
        modes.append(k_ref[rows, :] * m)
        modes.append(a_ref[rows, :] * m * (DT * HEAT))
        for n, v in enumerate(modes):
            cols_ref[pl.ds(8 * h * 32 + n, 8, stride=32), :] = v
    zero = jnp.zeros((3, 128), F32)
    acc = jnp.zeros((32, 128), F32)
    for c in range(16):
        cols_ref[c * 32 + 29 : c * 32 + 32, :] = zero
    for c in range(16):
        x, y = c // 4, c % 4
        start = y * 32 + x * 8
        v = pltpu.roll(cols_ref[c * 32 : c * 32 + 32, :], (4 + start) % 128, axis=1)
        acc = jnp.where((lane >= start) & (lane < start + 8), v, acc)
    zpay_ref[...] = acc


def by_parity(axis, write, first, second):
    even = lax.axis_index(axis) % 2 == 0

    @pl.when(even)
    def _():
        write(first, second)

    @pl.when(jnp.logical_not(even))
    def _():
        write(second, first)


def face_rows(cols_ref, c, axis, sign):
    base = c * 32
    if axis == 0:
        parts = [cols_ref[base + 9 * i : base + 9 * i + 9, :] for i in range(3)]
        return [parts[0] + parts[2] + sign * parts[1]]
    out = []
    for i in range(3):
        parts = [cols_ref[base + 9 * i + 3 * j : base + 9 * i + 3 * j + 3, :] for j in range(3)]
        out.append(parts[0] + parts[2] + sign * parts[1])
    return out


def put_faces(dst, at, cols_ref, c, axis, sign):
    row = at
    for part in face_rows(cols_ref, c, axis, sign):
        dst[row : row + part.shape[0], :] = part
        row += part.shape[0]
    dst[row : row + 1, :] = cols_ref[c * 32 + 27 : c * 32 + 28, :]
    dst[row + 1 : at + 16, :] = jnp.zeros((at + 15 - row, 128), F32)


def xpay_kernel(cols_ref, za_ref, zb_ref, first_ref, second_ref, h_ref):
    even = lax.axis_index("gz") % 2 == 0
    idx = lane_iota(32) % 8
    za, zb = za_ref[...], zb_ref[...]
    upper = jnp.where(even, za, zb)
    lower = jnp.where(even, zb, za)
    own = jnp.where(idx < 4, lower, upper)
    h_ref[...] = own

    def write(upper_ref, lower_ref):
        for d in range(1, 4):
            for y in range(4):
                at = ((d - 1) * 4 + y) * 32
                upper_ref[at : at + 32, :] = cols_ref[((4 - d) * 4 + y) * 32 : ((4 - d) * 4 + y) * 32 + 32, :]
                lower_ref[at : at + 32, :] = cols_ref[((d - 1) * 4 + y) * 32 : ((d - 1) * 4 + y) * 32 + 32, :]
        for y in range(4):
            put_faces(upper_ref, 384 + 16 * y, cols_ref, y, 0, 1.0)
            put_faces(lower_ref, 384 + 16 * y, cols_ref, 12 + y, 0, -1.0)
        upper_ref[448:480, :] = own
        lower_ref[448:480, :] = own

    by_parity("gx", write, first_ref, second_ref)


def ypay_kernel(cols_ref, xa_ref, xb_ref, h_ref, first_ref, second_ref):
    even = lax.axis_index("gx") % 2 == 0

    def halo(side, at, rows):
        a, b = xa_ref[at : at + rows, :], xb_ref[at : at + rows, :]
        return jnp.where(even, b, a) if side == 0 else jnp.where(even, a, b)

    def write(upper_ref, lower_ref):
        for x in range(4):
            for d in range(1, 4):
                at = ((d - 1) * 4 + x) * 32
                upper_ref[at : at + 32, :] = cols_ref[(x * 4 + 4 - d) * 32 : (x * 4 + 4 - d) * 32 + 32, :]
                lower_ref[at : at + 32, :] = cols_ref[(x * 4 + d - 1) * 32 : (x * 4 + d - 1) * 32 + 32, :]
            put_faces(upper_ref, 384 + 16 * x, cols_ref, x * 4, 1, 1.0)
            put_faces(lower_ref, 384 + 16 * x, cols_ref, x * 4 + 3, 1, -1.0)
        for n, (side, xd, d) in enumerate(CORNERS):
            at = 448 + 32 * n
            upper_ref[at : at + 32, :] = halo(side, ((xd - 1) * 4 + 4 - d) * 32, 32)
            lower_ref[at : at + 32, :] = halo(side, ((xd - 1) * 4 + d - 1) * 32, 32)
        for n, block in enumerate((halo(0, 448, 32), h_ref[...], halo(1, 448, 32))):
            upper_ref[832 + 32 * n : 864 + 32 * n, :] = block
            lower_ref[832 + 32 * n : 864 + 32 * n, :] = block

    by_parity("gy", write, first_ref, second_ref)


def couple(k1, k2):
    return (2.0 * PENALTY * DT) * k1 * k2 / jnp.maximum(k1 + k2, 1.0)


def roll_lanes(v, shift):
    return pltpu.roll(v, shift, axis=1)


def wide(v, n):
    return v if n == 8 else jnp.concatenate([v, v], axis=0)


def shift_rows(v, up):
    n = v.shape[0]
    amount, edge = (7, 7) if up else (1, 0)
    if n == 8:
        return pltpu.roll(v, amount, axis=0)
    a, b = pltpu.roll(v[0:8], amount, axis=0), pltpu.roll(v[8:16], amount, axis=0)
    take = row_iota(8) == edge
    return jnp.concatenate([jnp.where(take, b, a), jnp.where(take, a, b)], axis=0)


def line_faces(values, stride):
    out = []
    for base in range(27):
        if base // stride % 3 == 0:
            e = values[base] + values[base + 2 * stride]
            out.append((e - values[base + stride], e + values[base + stride]))
    return out


def slot(y):
    return (y + 2) % 16


def advance(values, kappa, heats, yz, fluxes):
    factor = {}
    for total in sorted({LAM[i] + LAM[j] + LAM[l] for i in range(3) for j in range(3) for l in range(3)}):
        factor[total] = 1.0 - kappa * total if total else None
    terms = []
    for lines in fluxes:
        per = []
        for low, high in lines:
            gain, both = low - high, low + high
            per.append((gain, -3.0 * both, 2.0 * gain))
        terms.append(per)
    out = []
    for i in range(3):
        for j in range(3):
            for l in range(3):
                v = values[mode(i, j, l)]
                f = factor[LAM[i] + LAM[j] + LAM[l]]
                v = v if f is None else v * f
                v = v + heats[i] * yz[3 * j + l]
                v = v + (terms[0][3 * j + l][i] + terms[1][3 * i + l][j]) + terms[2][3 * i + j][l]
                out.append(v)
    return out


def gauss_exp(offset, near, far):
    scaled = offset * jnp.where(offset >= 0.0, 1.0 / near, 1.0 / far)
    return jnp.exp(-3.0 * (scaled * scaled))


def main_kernel(
    cols_ref, h_ref, xa_ref, xb_ref, ya_ref, yb_ref, own_ref, cell_ref, lay_ref,
    t_out, pay_out,
    m0, m1, h0, h1, cx, cy, czu, czd, ch, yz, yzh, gs, q_ref, old, inc, amat, bmat, csum,
):
    gx, gy, gz = lax.axis_index("gx"), lax.axis_index("gy"), lax.axis_index("gz")
    even_x, even_y = gx % 2 == 0, gy % 2 == 0
    lane8 = lane_iota(8)
    idx8 = lane8 % 8

    zeros8 = jnp.zeros((8, 128), F32)

    def clear(n, _):
        m0[pl.ds(pl.multiple_of(n * 64, 64), 64), :] = jnp.zeros((64, 128), F32)
        return 0

    lax.fori_loop(0, 96, clear, 0)

    def place(x, y, block):
        m0[pl.ds((x + 4) * 512 + slot(y), 32, stride=16), :] = block

    def xhalo(side, at, rows):
        a, b = xa_ref[at : at + rows, :], xb_ref[at : at + rows, :]
        return jnp.where(even_x, b, a) if side == 0 else jnp.where(even_x, a, b)

    def yhalo(side, at, rows):
        a, b = ya_ref[at : at + rows, :], yb_ref[at : at + rows, :]
        return jnp.where(even_y, b, a) if side == 0 else jnp.where(even_y, a, b)

    for c in range(16):
        place(c // 4, c % 4, cols_ref[c * 32 : c * 32 + 32, :])
    for side in (0, 1):
        for d in range(1, 4):
            x = -d if side == 0 else 3 + d
            for y in range(4):
                place(x, y, xhalo(side, ((d - 1) * 4 + y) * 32, 32))
        x = -4 if side == 0 else 7
        for y in range(4):
            block = xhalo(side, 384 + 16 * y, 16)
            at = (x + 4) * 512 + slot(y)
            m0[pl.ds(at, 8, stride=16), :] = block[0:8]
            m0[pl.ds(at + 8 * 16, 1), :] = block[8:9]
            m0[pl.ds(at + 27 * 16, 1), :] = block[9:10]
    for side in (0, 1):
        for x in range(4):
            for d in range(1, 4):
                place(x, -d if side == 0 else 3 + d, yhalo(side, ((d - 1) * 4 + x) * 32, 32))
            block = yhalo(side, 384 + 16 * x, 16)
            at = (x + 4) * 512 + slot(-4 if side == 0 else 7)
            for i in range(3):
                for l in range(3):
                    m0[pl.ds(at + mode(i, 0, l) * 16, 1), :] = block[3 * i + l : 3 * i + l + 1]
            m0[pl.ds(at + 27 * 16, 1), :] = block[9:10]
        for n, (xside, xd, d) in enumerate(CORNERS):
            x = -xd if xside == 0 else 3 + xd
            place(x, -d if side == 0 else 3 + d, yhalo(side, 448 + 32 * n, 32))

    def clear_h(n, _):
        h0[pl.ds(pl.multiple_of(n * 64, 64), 64), :] = jnp.zeros((64, 128), F32)
        return 0

    lax.fori_loop(0, 8, clear_h, 0)
    lane32 = lane_iota(32)
    for yb in range(3):
        if yb == 1:
            blocks = [xhalo(0, 448, 32), h_ref[...], xhalo(1, 448, 32)]
        else:
            blocks = [yhalo(yb // 2, 832 + 32 * n, 32) for n in range(3)]
        for y in range(4):
            rolled = [roll_lanes(b, (32 * n - 32 * y) % 128) if (n - y) % 4 else b for n, b in enumerate(blocks)]
            v = jnp.where(lane32 < 32, rolled[0], jnp.where(lane32 < 64, rolled[1], rolled[2]))
            v = jnp.where(lane32 < 96, v, 0.0)
            h0[pl.ds(slot(4 * yb - 4 + y), 32, stride=16), :] = v

    lane16 = lane_iota(16)
    idx16 = lane16 % 8
    kh = h0[27 * 16 : 28 * 16, :]
    gk_src = jnp.where(idx16 == 5, roll_lanes(kh, 2), kh)
    ch[0:16, :] = couple(kh, roll_lanes(kh, 120))
    ch[16:32, :] = couple(kh, shift_rows(kh, True))
    ch[32:48, :] = jnp.where((idx16 == 3) | (idx16 == 7), 0.0, couple(kh, roll_lanes(kh, 127)))

    def kof(xi):
        return m0[pl.ds(pl.multiple_of(xi * 512 + 27 * 16, 16), 16), :]

    def couplings(xi, k):
        at = pl.multiple_of(xi * 16, 16)
        knext = kof(jnp.minimum(xi + 1, 11))
        gk = roll_lanes(gk_src, 123 - xi * 8)
        cx[pl.ds(at, 16), :] = couple(k, knext)
        cy[pl.ds(at, 16), :] = couple(k, shift_rows(k, True))
        czu[pl.ds(at, 16), :] = couple(k, jnp.where(lane16 == 127, gk, roll_lanes(k, 127)))
        czd[pl.ds(at, 16), :] = couple(k, gk)
        return knext

    lax.fori_loop(0, 11, couplings, kof(0))

    def line_modes(base, centre, near, far):
        return modal(*[gauss_exp(base + 0.5 * n - centre, near, far) for n in range(3)])

    s16 = row_iota(16)
    ypos = (gy * PY + jnp.where(s16 < 12, s16 - 2, s16 - 18)).astype(F32)
    ymodes = line_modes(ypos, NY * 0.5, NY / 4.0, NY / 4.0)
    zpos = (gz * PZ + lane16).astype(F32)
    zmodes = line_modes(zpos, NZ * 0.75, NZ / 8.0, NZ / 8.0)
    zhpos = (gz * PZ + jnp.where(idx16 < 4, idx16 - 4, idx16 + 124)).astype(F32)
    zhmodes = line_modes(zhpos, NZ * 0.75, NZ / 8.0, NZ / 8.0)
    for j in range(3):
        for l in range(3):
            at = (3 * j + l) * 16
            yz[at : at + 16, :] = ymodes[j] * zmodes[l]
            yzh[at : at + 16, :] = ymodes[j] * zhmodes[l]

    def rows_of(ref, xi, n):
        return [ref[pl.ds(pl.multiple_of(xi * 512 + 16 * m, 8), n), :] for m in range(27)]

    def at_x(ref, xi, n):
        return ref[pl.ds(pl.multiple_of(xi * 16, 8), n), :]

    def table(ref, n):
        return [ref[16 * t : 16 * t + n, :] for t in range(9)]

    s8 = row_iota(8)

    def pair(ref, p, m):
        a = ref[pl.ds((4 + 2 * p) * 512 + 16 * m, 8), :]
        b = ref[pl.ds((5 + 2 * p) * 512 + 16 * m, 8), :]
        return jnp.where(s8 < 4, pltpu.roll(a, 6, axis=0), pltpu.roll(b, 2, axis=0))

    low_modes = [mode(i, j, l) for i in range(2) for j in range(2) for l in range(2)]
    for g, m in enumerate(low_modes):
        for p in range(2):
            old[16 * g + 8 * p : 16 * g + 8 * p + 8, :] = pair(m0, p, m)

    groups = [
        [(1, 3, 8), (3, 9, 16), (9, 11, 8)],
        [(2, 4, 8), (4, 8, 16), (8, 10, 8)],
        [(3, 9, 8)],
        [(4, 8, 8)],
    ]
    src, dst, hsrc, hdst = m0, m1, h0, h1
    for step in range(STEPS):
        last = step == STEPS - 1
        centre_x = NX * 0.5 + step * NX / 16.0
        hn = 16 if step < 2 else 8
        hv = [hsrc[16 * m : 16 * m + hn, :] for m in range(27)]
        lane_h = lane_iota(hn)
        idx_h = lane_h % 8
        hz = line_faces(hv, 1)
        for t, (low, high) in enumerate(hz):
            gs[16 * t : 16 * t + hn, :] = jnp.where(idx_h == 5, roll_lanes(high, 2), low)
        if not last:
            for t in range(9):
                q_ref[8 * t : 8 * t + 8, :] = zeros8

        for first, end, n in groups[step]:
            lane_n = lane_iota(n)

            def xflux(here, there, xi, n=n):
                c = at_x(cx, xi, n)
                return tuple(c * (a[1] - b[0]) for a, b in zip(line_faces(here, 9), line_faces(there, 9)))

            def body(xi, carry, n=n, src=src, dst=dst, step=step, last=last, lane_n=lane_n, centre_x=centre_x):
                left = carry
                values = rows_of(src, xi, n)
                following = rows_of(src, xi + 1, n)
                right = xflux(values, following, xi, n)
                kappa = DT * src_k(xi, n)
                heat = src_a(xi, n)
                base = (gx * PX + xi - 4).astype(F32) - centre_x
                splat = jnp.full((8, 128), base, F32)
                xm = modal(*[gauss_exp(splat + 0.5 * t, NX / 8.0, NX / 4.0) for t in range(3)])
                heats = [heat * wide(v, n) for v in xm]
                c = at_x(cy, xi, n)
                yf = []
                for low, high in line_faces(values, 3):
                    up = c * (high - shift_rows(low, True))
                    yf.append((shift_rows(up, False), up))
                cu, cd = at_x(czu, xi, n), at_x(czd, xi, n)
                zf = []
                shift = 123 - xi * 8
                mine = (lane8 == xi * 8 + 4) | (lane8 == xi * 8 + 5)
                for t, (low, high) in enumerate(line_faces(values, 1)):
                    g = roll_lanes(gs[16 * t : 16 * t + n, :], shift)
                    up = cu * (high - jnp.where(lane_n == 127, g, roll_lanes(low, 127)))
                    down = jnp.where(lane_n == 0, cd * (g - low), roll_lanes(up, 1))
                    zf.append((down, up))
                    if not last:
                        back = roll_lanes(jnp.where(lane8 == 127, up[0:8], down[0:8]), xi * 8 + 5)
                        q_ref[8 * t : 8 * t + 8, :] = jnp.where(mine, back, q_ref[8 * t : 8 * t + 8, :])
                out = advance(values, kappa, heats, table(yz, n), (list(zip(left, right)), yf, zf))
                for m, v in enumerate(out):
                    dst[pl.ds(pl.multiple_of(xi * 512 + 16 * m, 8), n), :] = v
                return right

            def src_k(xi, n):
                return m0[pl.ds(pl.multiple_of(xi * 512 + 27 * 16, 8), n), :]

            def src_a(xi, n):
                return m0[pl.ds(pl.multiple_of(xi * 512 + 28 * 16, 8), n), :]

            left = xflux(rows_of(src, first - 1, n), rows_of(src, first, n), first - 1, n)
            lax.fori_loop(first, end, body, left)

        if not last:
            n = 16 if step == 0 else 8
            hv = [v[0:n] for v in hv]
            idx_n = lane_iota(n) % 8
            xpos = (gx * PX + lane_iota(8) // 8 - 4).astype(F32) - centre_x
            xm = modal(*[gauss_exp(xpos + 0.5 * t, NX / 8.0, NX / 4.0) for t in range(3)])
            heat = h0[28 * 16 : 28 * 16 + n, :]
            heats = [heat * wide(v, n) for v in xm]
            c = ch[0:n, :]
            xf = []
            for low, high in line_faces(hv, 9):
                up = c * (high - roll_lanes(low, 120))
                xf.append((roll_lanes(up, 8), up))
            c = ch[16 : 16 + n, :]
            yf = []
            for low, high in line_faces(hv, 3):
                up = c * (high - shift_rows(low, True))
                yf.append((shift_rows(up, False), up))
            c = ch[32 : 32 + n, :]
            zf = []
            for t, (low, high) in enumerate(line_faces(hv, 1)):
                up = c * (high - roll_lanes(low, 127))
                q = wide(q_ref[8 * t : 8 * t + 8, :], n)
                down = jnp.where(idx_n == 4, q, roll_lanes(up, 1))
                zf.append((down, jnp.where(idx_n == 3, roll_lanes(q, 126), up)))
            kappa = DT * h0[27 * 16 : 27 * 16 + n, :]
            out = advance(hv, kappa, heats, table(yzh, n), (xf, yf, zf))
            for m, v in enumerate(out):
                hdst[16 * m : 16 * m + n, :] = v
        src, dst, hsrc, hdst = dst, src, hdst, hsrc

    live = (lane8 < lay_ref[0]).astype(F32)
    for p in range(2):
        modes = [pair(src, p, m) for m in range(27)]
        for g, m in enumerate(low_modes):
            at = 16 * g + 8 * p
            inc[at : at + 8, :] = (modes[m] - old[at : at + 8, :]) * live
        for n, v in enumerate(nodal_grid(modes)):
            t_out[n, 8 * p : 8 * p + 8, :] = v

    ones = row_iota(16)
    for c in range(16):
        lanes = slice(128 * c, 128 * c + 128)
        v = inc[pl.ds(c, 8, stride=16), :]
        hi = v.astype(jnp.bfloat16).astype(F32)
        lo = v - hi
        owner = jnp.broadcast_to(own_ref[c : c + 1, :], (8, 128))
        picks = [owner == o for o in range(OWNERS)]
        amat[0:128, lanes] = jnp.concatenate([jnp.where(k, hi, 0.0) for k in picks], axis=0).astype(jnp.bfloat16)
        amat[128:256, lanes] = jnp.concatenate([jnp.where(k, lo, 0.0) for k in picks], axis=0).astype(jnp.bfloat16)
        owner16 = jnp.broadcast_to(own_ref[c : c + 1, :], (16, 128))
        amat[256:272, lanes] = jnp.where(owner16 == ones, wide(live, 16), 0.0).astype(jnp.bfloat16)
        cell = jnp.broadcast_to(cell_ref[c : c + 1, :], (CELLS, 128))
        hit = cell == row_iota(CELLS)
        bmat[:, lanes] = jnp.where(hit, 1.0, 0.0).astype(jnp.bfloat16)
    total = lax.dot_general(
        amat[...], bmat[...], (((1,), (1,)), ((), ())), preferred_element_type=F32
    )
    csum[0:128, :] = (total[0:128] + total[128:256])[:, 0:128]
    csum[128:256, :] = (total[0:128] + total[128:256])[:, 128:256]
    for h in range(2):
        for g in range(8):
            pay_out[pl.ds(2 * g + h, 16, stride=18), :] = csum[pl.ds(128 * h + g, 16, stride=8), :]
        pay_out[pl.ds(16 + h, 16, stride=18), :] = total[256:272, 128 * h : 128 * h + 128]


def gradient_table():
    spots = [0.5 - 0.5 / math.sqrt(3.0), 0.5 + 0.5 / math.sqrt(3.0)]
    out = np.zeros((3, 8, 8), np.float32)
    for node in range(8):
        corner = [node // 4, node // 2 % 2, node % 2]
        for point in range(8):
            place = [spots[point // 4], spots[point // 2 % 2], spots[point % 2]]
            values = [place[k] if corner[k] else 1.0 - place[k] for k in range(3)]
            slopes = [1.0 if corner[k] else -1.0 for k in range(3)]
            out[0, node, point] = slopes[0] * values[1] * values[2] / 8.0
            out[1, node, point] = values[0] * slopes[1] * values[2] / 8.0
            out[2, node, point] = values[0] * values[1] * slopes[2] / 8.0
    return out


def column(values):
    rows = row_iota(8)
    out = jnp.full((8, 128), float(values[7]), F32)
    for r in range(7):
        out = jnp.where(rows == r, float(values[r]), out)
    return out


def mechanics_kernel(got_ref, de_ref, st_ref, lim_ref, stress_out, force_out):
    sums = got_ref[0:18, :]
    for s in range(1, OWNERS):
        sums = sums + got_ref[18 * s : 18 * s + 18, :]
    root = 1.0 / math.sqrt(3.0)
    rows = row_iota(8)
    signs = [jnp.where(rows // w % 2 == 0, -root, root) for w in (4, 2, 1)]
    table = gradient_table()
    cols = [[column(table[d, :, g]) for g in range(8)] for d in range(3)]
    for h in range(2):
        lanes = slice(128 * h, 128 * h + 128)
        inv = 1.0 / jnp.maximum(sums[16 + h : 17 + h], 1.0)

        def row(m):
            return jnp.broadcast_to(sums[2 * m + h : 2 * m + h + 1] * inv, (8, 128))

        z = [row(2 * n) + signs[2] * row(2 * n + 1) for n in range(4)]
        y = [z[2 * n] + signs[1] * z[2 * n + 1] for n in range(2)]
        strain = EXPANSION * (y[0] + signs[0] * y[1])
        normal = [de_ref[k, :, lanes] - strain for k in range(3)]
        volume = normal[0] + normal[1] + normal[2]
        trial = [st_ref[k, :, lanes] + LAME * volume + 2.0 * MU * normal[k] for k in range(3)]
        shear = [st_ref[k, :, lanes] + 2.0 * MU * de_ref[k, :, lanes] for k in range(3, 6)]
        pressure = (trial[0] + trial[1] + trial[2]) * (1.0 / 3.0)
        dev = [t - pressure for t in trial]
        squares = dev[0] * dev[0] + dev[1] * dev[1] + dev[2] * dev[2]
        squares = squares + 2.0 * (shear[0] * shear[0] + shear[1] * shear[1] + shear[2] * shear[2])
        equivalent = jnp.sqrt(1.5 * squares)
        limit = jnp.broadcast_to(lim_ref[0:1, lanes], (8, 128))
        plastic = jnp.maximum(equivalent - limit, 0.0) * (1.0 / (3.0 * MU + HARD))
        factor = 1.0 - (3.0 * MU) * plastic / jnp.maximum(equivalent, limit)
        stress = [pressure + factor * d for d in dev] + [factor * s for s in shear]
        for k in range(6):
            stress_out[k, :, lanes] = stress[k]
        index = [[0, 5, 4], [5, 1, 3], [4, 3, 2]]
        forces = [jnp.zeros((8, 128), F32)] * 3
        for g in range(8):
            at = [jnp.broadcast_to(s[g : g + 1], (8, 128)) for s in stress]
            for c in range(3):
                for d in range(3):
                    forces[c] = forces[c] + cols[d][g] * at[index[c][d]]
        for c in range(3):
            force_out[c, :, lanes] = forces[c]


def swap(first, second, axis, count):
    even = [(i, i ^ 1) for i in range(count)]
    odd = [(i, i + 1 if i % 2 else i - 1) for i in range(1, count - 1)]
    return lax.ppermute(first, axis, even), lax.ppermute(second, axis, odd)


def local(temps, cond, absorb, layers, owner, cell, de, st, lim):
    rows = lambda n: pltpu.VMEM((n, 128), F32)
    sx, sy, sz = (lax.axis_size(a) for a in ("gx", "gy", "gz"))
    temps = temps.reshape(27, 16, 128)
    layers = layers.reshape(1)
    cols, zpay = call(
        prep_kernel,
        (rows(512), rows(32)),
        (temps, cond.reshape(16, 128), absorb.reshape(16, 128), layers),
        smem=(3,),
    )
    za, zb = swap(zpay, zpay, "gz", sz)
    xf, xs, hown = call(xpay_kernel, (rows(XROWS), rows(XROWS), rows(32)), (cols, za, zb), near=(0, 1, 2))
    xa, xb = swap(xf, xs, "gx", sx)
    yf, ys = call(ypay_kernel, (rows(YROWS), rows(YROWS)), (cols, xa, xb, hown), near=(0, 1, 2, 3))
    ya, yb = swap(yf, ys, "gy", sy)
    vm = lambda n: pltpu.VMEM((n, 128), F32)
    t_new, pay = call(
        main_kernel,
        (jax.ShapeDtypeStruct((27, 16, 128), F32), rows(OWNERS * 18)),
        (cols, hown, xa, xb, ya, yb, owner.reshape(16, 128), cell.reshape(16, 128), layers),
        scratch=[
            vm(6144), vm(6144), vm(512), vm(512),
            vm(192), vm(192), vm(192), vm(192), vm(48), vm(144), vm(144), vm(144), vm(72), vm(128), vm(128),
            pltpu.VMEM((272, 2048), jnp.bfloat16), pltpu.VMEM((256, 2048), jnp.bfloat16), vm(256),
        ],
        smem=(8,),
        near=(0, 1, 2, 3, 4, 5),
    )
    got = lax.all_to_all(pay.reshape(OWNERS, 1, 2304), "gx", 0, 0, tiled=True)
    stress, forces = call(
        mechanics_kernel,
        (jax.ShapeDtypeStruct((6, 8, 256), F32), jax.ShapeDtypeStruct((3, 8, 256), F32)),
        (got.reshape(OWNERS * 18, 128), de, st, lim.reshape(1, 256)),
        near=(0,),
    )
    return t_new.reshape(3, 3, 3, 4, 4, 128), stress, forces


def solution(mesh):
    cells = P(None, None, ("gx", "gy", "gz"))
    temps = P(None, None, None, "gx", "gy", "gz")
    block = P("gx", "gy", "gz")
    return jax.shard_map(
        local,
        mesh=mesh,
        in_specs=(
            temps, block, block, block, P("gx", "gy", "gz", None, None), P("gx", "gy", "gz", None),
            cells, cells, P(("gx", "gy", "gz")),
        ),
        out_specs=(temps, cells, cells),
        check_vma=False,
    )
```

```python
import functools
import math

import jax
import jax.numpy as jnp
import numpy as np
from jax import lax
from jax.experimental import pallas as pl
from jax.experimental.pallas import tpu as pltpu
from jax.sharding import PartitionSpec as P


STEPS = 4
DT = 0.003
PENALTY = 3.0
HEAT = 100.0 * (2.0 / 3.0)
EXPANSION = 0.02
MU = 100.0 / 2.6
LAME = 30.0 / 0.52
HARD = 10.0
NX, NY, NZ = 64, 32, 512
PX, PY, PZ = 4, 4, 128
OWNERS, CELLS = 16, 256
F32 = jnp.float32

LAM = (0.0, 12.0, 24.0)
ROWS = 29

XFULL = {(d, y): ((d - 1) * 4 + y) * ROWS for d in (1, 2, 3) for y in range(4)}
XFACE = [12 * ROWS + 10 * y for y in range(4)]
XH = 12 * ROWS + 40
XROWS = 424
YFULL = {(d, x): ((d - 1) * 4 + x) * ROWS for d in (1, 2, 3) for x in range(4)}
YFACE = [12 * ROWS + 10 * x for x in range(4)]
NEAR = [(side, xd, d) for side in (0, 1) for xd in (1, 2) for d in range(1, 4 - xd)]
EDGE = [(side, xd, 4 - xd) for side in (0, 1) for xd in (1, 2, 3)]
YNEAR = [12 * ROWS + 40 + ROWS * n for n in range(6)]
YEDGE = [18 * ROWS + 40 + 16 * n for n in range(6)]
YH = [18 * ROWS + 136, 19 * ROWS + 136]
YROWS = 720


def mode(i, j, l):
    return 9 * i + 3 * j + l


def call(kernel, outs, args, scratch=(), far=(), aliases=None):
    def place(n, a):
        return a if a.size == 1 else pltpu.with_memory_space_constraint(a, pltpu.HBM if n in far else pltpu.VMEM)

    return pl.pallas_call(
        kernel,
        out_shape=outs,
        in_specs=[
            pl.BlockSpec(memory_space=pltpu.SMEM if a.size == 1 else pltpu.HBM if n in far else pltpu.VMEM)
            for n, a in enumerate(args)
        ],
        out_specs=tuple(pl.BlockSpec(memory_space=o.memory_space) for o in outs),
        input_output_aliases=aliases or {},
        compiler_params=pltpu.CompilerParams(vmem_limit_bytes=24 << 20),
        scratch_shapes=list(scratch),
    )(*[place(n, a) for n, a in enumerate(args)])


def fetch(pairs, sems):
    copies = [pltpu.make_async_copy(a, b, sems.at[n]) for n, (a, b) in enumerate(pairs)]
    for c in copies:
        c.start()
    for c in copies:
        c.wait()


def lane_iota(rows):
    return lax.broadcasted_iota(jnp.int32, (rows, 128), 1)


def row_iota(rows):
    return lax.broadcasted_iota(jnp.int32, (rows, 128), 0)


def modal(a, b, c):
    s = a + c
    return (s + 4.0 * b) * (1.0 / 6.0), (c - a) * 0.5, (s - 2.0 * b) * (1.0 / 3.0)


def modal_grid(values):
    for stride in (9, 3, 1):
        out = [None] * 27
        for base in range(27):
            if base // stride % 3 == 0:
                ids = [base + stride * t for t in range(3)]
                for q, r in zip(ids, modal(*[values[q] for q in ids])):
                    out[q] = r
        values = out
    return values


def nodal_grid(values):
    for stride in (9, 3, 1):
        out = [None] * 27
        for base in range(27):
            if base // stride % 3 == 0:
                al, be, ga = (values[base + stride * t] for t in range(3))
                e = al + ga
                out[base], out[base + stride], out[base + 2 * stride] = e - be, al - 0.5 * ga, e + be
        values = out
    return values


def prep_kernel(t_in, k_in, a_in, lay_ref, cols_ref, zpay_ref, live_ref, t_ref, k_ref, a_ref, sems):
    fetch(((t_in, t_ref), (k_in, k_ref), (a_in, a_ref)), sems)
    m = (lane_iota(8) < lay_ref[0, 0, 0]).astype(F32)
    live_ref[...] = m
    lane = lane_iota(32)
    for h in range(2):
        rows = slice(8 * h, 8 * h + 8)
        modes = modal_grid([t_ref[n, rows, :] for n in range(27)])
        modes.append(k_ref[rows, :] * m)
        modes.append(a_ref[rows, :] * m * (DT * HEAT))
        for n, v in enumerate(modes):
            cols_ref[pl.ds(8 * h * 32 + n, 8, stride=32), :] = v
    zero = jnp.zeros((3, 128), F32)
    acc = jnp.zeros((32, 128), F32)
    for c in range(16):
        cols_ref[c * 32 + 29 : c * 32 + 32, :] = zero
    for c in range(16):
        x, y = c // 4, c % 4
        start = y * 32 + x * 8
        v = pltpu.roll(cols_ref[c * 32 : c * 32 + 32, :], (4 + start) % 128, axis=1)
        acc = jnp.where((lane >= start) & (lane < start + 8), v, acc)
    zpay_ref[...] = acc


def by_parity(axis, write, first, second):
    even = lax.axis_index(axis) % 2 == 0

    @pl.when(even)
    def _():
        write(first, second)

    @pl.when(jnp.logical_not(even))
    def _():
        write(second, first)


def face_rows(cols_ref, c, axis, sign):
    base = c * 32
    if axis == 0:
        parts = [cols_ref[base + 9 * i : base + 9 * i + 9, :] for i in range(3)]
        return [parts[0] + parts[2] + sign * parts[1]]
    out = []
    for i in range(3):
        parts = [cols_ref[base + 9 * i + 3 * j : base + 9 * i + 3 * j + 3, :] for j in range(3)]
        out.append(parts[0] + parts[2] + sign * parts[1])
    return out


def put_faces(dst, at, cols_ref, c, axis, sign):
    row = at
    for part in face_rows(cols_ref, c, axis, sign):
        dst[row : row + part.shape[0], :] = part
        row += part.shape[0]
    dst[row : row + 1, :] = cols_ref[c * 32 + 27 : c * 32 + 28, :]


def xhalo_block(even, xa_ref, xb_ref, side, at, rows):
    a, b = xa_ref[at : at + rows, :], xb_ref[at : at + rows, :]
    return jnp.where(even, b, a) if side == 0 else jnp.where(even, a, b)


def xpay_kernel(cols_ref, za_ref, zb_ref, first_ref, second_ref, h_ref):
    even = lax.axis_index("gz") % 2 == 0
    idx = lane_iota(32) % 8
    za, zb = za_ref[...], zb_ref[...]
    upper = jnp.where(even, za, zb)
    lower = jnp.where(even, zb, za)
    own = jnp.where(idx < 4, lower, upper)
    h_ref[...] = own

    def write(upper_ref, lower_ref):
        for (d, y), at in XFULL.items():
            up, down = ((4 - d) * 4 + y) * 32, ((d - 1) * 4 + y) * 32
            upper_ref[at : at + ROWS, :] = cols_ref[up : up + ROWS, :]
            lower_ref[at : at + ROWS, :] = cols_ref[down : down + ROWS, :]
        for y in range(4):
            put_faces(upper_ref, XFACE[y], cols_ref, y, 0, 1.0)
            put_faces(lower_ref, XFACE[y], cols_ref, 12 + y, 0, -1.0)
        for ref in (upper_ref, lower_ref):
            ref[XH : XH + ROWS, :] = own[0:ROWS]

    by_parity("gx", write, first_ref, second_ref)


def ypay_kernel(cols_ref, xa_ref, xb_ref, h_ref, first_ref, second_ref):
    halo = functools.partial(xhalo_block, lax.axis_index("gx") % 2 == 0, xa_ref, xb_ref)

    def corner(side, at, ysign):
        xsign = 1.0 if side == 0 else -1.0
        c = [halo(side, at + 9 * i, 9) for i in range(3)]
        xface = c[0] + c[2] + xsign * c[1]
        yface = [v[0:3] + v[6:9] + ysign * v[3:6] for v in c[1:]]
        return (xface[0:3] - xsign * yface[0] - yface[1], xface[3:9], yface[0], yface[1], halo(side, at + 27, 1))

    def write(upper_ref, lower_ref):
        for (d, x), at in YFULL.items():
            up, down = (x * 4 + 4 - d) * 32, (x * 4 + d - 1) * 32
            upper_ref[at : at + ROWS, :] = cols_ref[up : up + ROWS, :]
            lower_ref[at : at + ROWS, :] = cols_ref[down : down + ROWS, :]
        for x in range(4):
            put_faces(upper_ref, YFACE[x], cols_ref, x * 4, 1, 1.0)
            put_faces(lower_ref, YFACE[x], cols_ref, x * 4 + 3, 1, -1.0)
        for (side, xd, d), at in zip(NEAR, YNEAR):
            upper_ref[at : at + ROWS, :] = halo(side, XFULL[xd, 4 - d], ROWS)
            lower_ref[at : at + ROWS, :] = halo(side, XFULL[xd, d - 1], ROWS)
        for (side, xd, d), at in zip(EDGE, YEDGE):
            for ref, y, sign in ((upper_ref, 4 - d, 1.0), (lower_ref, d - 1, -1.0)):
                row = at
                for part in corner(side, XFULL[xd, y], sign):
                    ref[row : row + part.shape[0], :] = part
                    row += part.shape[0]
        beside = jnp.where(lane_iota(ROWS) // 8 % 4 < 2, halo(1, XH, ROWS), halo(0, XH, ROWS))
        for ref in (upper_ref, lower_ref):
            ref[YH[0] : YH[0] + ROWS, :] = h_ref[0:ROWS, :]
            ref[YH[1] : YH[1] + ROWS, :] = beside

    by_parity("gy", write, first_ref, second_ref)


def couple(k1, k2):
    return (2.0 * PENALTY * DT) * k1 * k2 / jnp.maximum(k1 + k2, 1.0)


def roll_lanes(v, shift):
    return pltpu.roll(v, shift, axis=1)


def wide(v, n):
    return v if n == 8 else jnp.concatenate([v, v], axis=0)


def shift_rows(v, up):
    n = v.shape[0]
    amount, edge = (7, 7) if up else (1, 0)
    if n == 8:
        return pltpu.roll(v, amount, axis=0)
    a, b = pltpu.roll(v[0:8], amount, axis=0), pltpu.roll(v[8:16], amount, axis=0)
    take = row_iota(8) == edge
    return jnp.concatenate([jnp.where(take, b, a), jnp.where(take, a, b)], axis=0)


def line_faces(values, stride):
    out = []
    for base in range(27):
        if base // stride % 3 == 0:
            e = values[base] + values[base + 2 * stride]
            out.append((e - values[base + stride], e + values[base + stride]))
    return out


def slot(y):
    return (y + 2) % 16


def advance(values, kappa, heats, yz, fluxes):
    factor = {}
    for total in sorted({LAM[i] + LAM[j] + LAM[l] for i in range(3) for j in range(3) for l in range(3)}):
        factor[total] = 1.0 - kappa * total if total else None
    terms = []
    for lines in fluxes:
        per = []
        for low, high in lines:
            gain, both = low - high, low + high
            per.append((gain, -3.0 * both, 2.0 * gain))
        terms.append(per)
    out = []
    for i in range(3):
        for j in range(3):
            for l in range(3):
                v = values[mode(i, j, l)]
                f = factor[LAM[i] + LAM[j] + LAM[l]]
                v = v if f is None else v * f
                v = v + heats[i] * yz[3 * j + l]
                v = v + (terms[0][3 * j + l][i] + terms[1][3 * i + l][j]) + terms[2][3 * i + j][l]
                out.append(v)
    return out


def gauss_exp(offset, near, far):
    scaled = offset * jnp.where(offset >= 0.0, 1.0 / near, 1.0 / far)
    return jnp.exp(-3.0 * (scaled * scaled))


def place(m0, x, y, block):
    m0[pl.ds((x + 4) * 512 + slot(y), ROWS, stride=16), :] = block


def place_h(h0, row, y, blocks):
    lane = lane_iota(ROWS)
    rolled = [roll_lanes(b, (32 * n - 32 * y) % 128) if (n - y) % 4 else b for n, b in enumerate(blocks)]
    v = jnp.where(lane < 32, rolled[0], jnp.where(lane < 64, rolled[1], rolled[2]))
    h0[pl.ds(row, ROWS, stride=16), :] = jnp.where(lane < 96, v, 0.0)


def pair(ref, p, m):
    a = ref[pl.ds((4 + 2 * p) * 512 + 16 * m, 8), :]
    b = ref[pl.ds((5 + 2 * p) * 512 + 16 * m, 8), :]
    return jnp.where(row_iota(8) < 4, pltpu.roll(a, 6, axis=0), pltpu.roll(b, 2, axis=0))


LOW = [mode(i, j, l) for i in range(2) for j in range(2) for l in range(2)]


def line_modes(base, centre, near, far):
    return modal(*[gauss_exp(base + 0.5 * n - centre, near, far) for n in range(3)])


def pre_kernel(
    cols_ref, h_ref, xa_ref, xb_ref, own_in, cell_in,
    m0, h0, yz, yzh, xtab, xhtab, old, bmat, own_out,
    cell_ref, sems,
):
    gx, gy, gz = lax.axis_index("gx"), lax.axis_index("gy"), lax.axis_index("gz")
    even_x = gx % 2 == 0
    fetch(((own_in, own_out), (cell_in, cell_ref)), sems)

    def clear(n, _):
        m0[pl.ds(pl.multiple_of(n * 128, 128), 128), :] = jnp.zeros((128, 128), F32)
        return 0

    lax.fori_loop(0, 48, clear, 0)
    h0[...] = jnp.zeros((512, 128), F32)
    xhalo = functools.partial(xhalo_block, even_x, xa_ref, xb_ref)
    for c in range(16):
        place(m0, c // 4, c % 4, cols_ref[c * 32 : c * 32 + ROWS, :])
    for side in (0, 1):
        for d in range(1, 4):
            x = -d if side == 0 else 3 + d
            for y in range(4):
                place(m0, x, y, xhalo(side, XFULL[d, y], ROWS))
        x = -4 if side == 0 else 7
        for y in range(4):
            block = xhalo(side, XFACE[y], 10)
            at = (x + 4) * 512 + slot(y)
            m0[pl.ds(at, 8, stride=16), :] = block[0:8]
            m0[pl.ds(at + 8 * 16, 1), :] = block[8:9]
            m0[pl.ds(at + 27 * 16, 1), :] = block[9:10]
    blocks = [xhalo(0, XH, ROWS), h_ref[0:ROWS, :], xhalo(1, XH, ROWS)]
    for y in range(4):
        place_h(h0, slot(y), y, blocks)

    lane16 = lane_iota(16)
    idx16 = lane16 % 8
    s16 = row_iota(16)
    ypos = (gy * PY + jnp.where(s16 < 12, s16 - 2, s16 - 18)).astype(F32)
    ymodes = line_modes(ypos, NY * 0.5, NY / 4.0, NY / 4.0)
    zpos = (gz * PZ + lane16).astype(F32)
    zmodes = line_modes(zpos, NZ * 0.75, NZ / 8.0, NZ / 8.0)
    zhpos = (gz * PZ + jnp.where(idx16 < 4, idx16 - 4, idx16 + 124)).astype(F32)
    zhmodes = line_modes(zhpos, NZ * 0.75, NZ / 8.0, NZ / 8.0)
    for j in range(3):
        for l in range(3):
            at = (3 * j + l) * 16
            yz[at : at + 16, :] = ymodes[j] * zmodes[l]
            yzh[at : at + 16, :] = ymodes[j] * zhmodes[l]
    for step in range(STEPS):
        centre = NX * 0.5 + step * NX / 16.0
        for t, v in enumerate(line_modes((gx * PX + s16 - 4).astype(F32), centre, NX / 8.0, NX / 4.0)):
            xtab[(3 * step + t) * 16 : (3 * step + t) * 16 + 16, :] = v
        for t, v in enumerate(line_modes((gx * PX + lane_iota(8) // 8 - 4).astype(F32), centre, NX / 8.0, NX / 4.0)):
            xhtab[(3 * step + t) * 8 : (3 * step + t) * 8 + 8, :] = v

    for g, m in enumerate(LOW):
        for p in range(2):
            old[16 * g + 8 * p : 16 * g + 8 * p + 8, :] = pair(m0, p, m)
    for c in range(16):
        cell = jnp.broadcast_to(cell_ref[c : c + 1, :], (CELLS, 128))
        hit = cell == row_iota(CELLS)
        bmat[:, 128 * c : 128 * c + 128] = jnp.where(hit, 1.0, 0.0).astype(jnp.bfloat16)


def main_kernel(
    m0_in, h0_in, yz, yzh, xtab, xhtab, old, bmat, xa_ref, xb_ref, ya_ref, yb_ref, h_ref, own_ref, live_ref,
    t_hbm, pay_out, m0, h0,
    t_out, sem, m1, h1, cx, cy, czu, czd, ch, gs, q_ref, inc, amat, csum,
):
    del m0_in, h0_in
    even_y = lax.axis_index("gy") % 2 == 0
    lane8 = lane_iota(8)
    zeros8 = jnp.zeros((8, 128), F32)

    def yhalo(side, at, rows):
        a, b = ya_ref[at : at + rows, :], yb_ref[at : at + rows, :]
        return jnp.where(even_y, b, a) if side == 0 else jnp.where(even_y, a, b)

    for side in (0, 1):
        out = [-d if side == 0 else 3 + d for d in range(5)]
        for (d, x), at in YFULL.items():
            place(m0, x, out[d], yhalo(side, at, ROWS))
        for x in range(4):
            block = yhalo(side, YFACE[x], 10)
            at = (x + 4) * 512 + slot(out[4])
            for i in range(3):
                for l in range(3):
                    m0[pl.ds(at + mode(i, 0, l) * 16, 1), :] = block[3 * i + l : 3 * i + l + 1]
            m0[pl.ds(at + 27 * 16, 1), :] = block[9:10]
        for (xside, xd, d), at in zip(NEAR, YNEAR):
            place(m0, -xd if xside == 0 else 3 + xd, out[d], yhalo(side, at, ROWS))
        for (xside, xd, d), at in zip(EDGE, YEDGE):
            block = yhalo(side, at, 16)
            to = ((-xd if xside == 0 else 3 + xd) + 4) * 512 + slot(out[d])
            m0[pl.ds(to, 8, stride=16), :] = block[0:8]
            for row, m in enumerate((8, 9, 10, 11, 18, 19, 20, 27), 8):
                m0[pl.ds(to + 16 * m, 1), :] = block[row : row + 1]
        beside = yhalo(side, YH[1], ROWS)
        blocks = [beside, yhalo(side, YH[0], ROWS), beside]
        for y in range(4):
            place_h(h0, slot(8 * side - 4 + y), y, blocks)

    lane16 = lane_iota(16)
    idx16 = lane16 % 8
    kh = h0[27 * 16 : 28 * 16, :]
    gk_src = jnp.where(idx16 == 5, roll_lanes(kh, 2), kh)
    ch[0:16, :] = couple(kh, roll_lanes(kh, 120))
    ch[16:32, :] = couple(kh, shift_rows(kh, True))
    ch[32:48, :] = jnp.where((idx16 == 3) | (idx16 == 7), 0.0, couple(kh, roll_lanes(kh, 127)))

    def kof(xi, n):
        return m0[xi * 512 + 27 * 16 : xi * 512 + 27 * 16 + n, :]

    for xi in range(11):
        n = 16 if 2 <= xi < 9 else 8
        at = slice(xi * 16, xi * 16 + n)
        k = kof(xi, n)
        cx[at, :] = couple(k, kof(xi + 1, n))
        if xi == 0:
            continue
        gk = roll_lanes(gk_src[0:n], (123 - xi * 8) % 128)
        cy[at, :] = couple(k, shift_rows(k, True))
        czu[at, :] = couple(k, jnp.where(lane_iota(n) == 127, gk, roll_lanes(k, 127)))
        czd[at, :] = couple(k, gk)

    def rows_of(ref, xi, n):
        return [ref[pl.ds(pl.multiple_of(xi * 512 + 16 * m, 8), n), :] for m in range(27)]

    def at_x(ref, xi, n):
        return ref[pl.ds(pl.multiple_of(xi * 16, 8), n), :]

    def table(ref, n):
        return [ref[16 * t : 16 * t + n, :] for t in range(9)]

    groups = [
        [(1, 3, 8), (3, 9, 16), (9, 11, 8)],
        [(2, 4, 8), (4, 8, 16), (8, 10, 8)],
        [(3, 9, 8)],
        [(4, 8, 8)],
    ]
    src, dst, hsrc, hdst = m0, m1, h0, h1
    for step in range(STEPS):
        last = step == STEPS - 1
        hn = 16 if step < 2 else 8
        hv = [hsrc[16 * m : 16 * m + hn, :] for m in range(27)]
        lane_h = lane_iota(hn)
        idx_h = lane_h % 8
        hz = line_faces(hv, 1)
        for t, (low, high) in enumerate(hz):
            gs[16 * t : 16 * t + hn, :] = jnp.where(idx_h == 5, roll_lanes(high, 2), low)
        if not last:
            for t in range(9):
                q_ref[8 * t : 8 * t + 8, :] = zeros8

        for first, end, n in groups[step]:
            lane_n = lane_iota(n)

            def xflux(here, there, xi, n=n):
                c = at_x(cx, xi, n)
                return tuple(c * (a[1] - b[0]) for a, b in zip(line_faces(here, 9), line_faces(there, 9)))

            def body(xi, carry, n=n, src=src, dst=dst, step=step, last=last, lane_n=lane_n):
                left = carry
                values = rows_of(src, xi, n)
                following = rows_of(src, xi + 1, n)
                right = xflux(values, following, xi, n)
                kappa = DT * src_k(xi, n)
                heat = src_a(xi, n)
                xm = [xtab[pl.ds((3 * step + t) * 16 + xi, 1), :] for t in range(3)]
                heats = [heat * jnp.broadcast_to(v, (n, 128)) for v in xm]
                c = at_x(cy, xi, n)
                yf = []
                for low, high in line_faces(values, 3):
                    up = c * (high - shift_rows(low, True))
                    yf.append((shift_rows(up, False), up))
                cu, cd = at_x(czu, xi, n), at_x(czd, xi, n)
                zf = []
                shift = 123 - xi * 8
                mine = (lane8 == xi * 8 + 4) | (lane8 == xi * 8 + 5)
                for t, (low, high) in enumerate(line_faces(values, 1)):
                    g = roll_lanes(gs[16 * t : 16 * t + n, :], shift)
                    up = cu * (high - jnp.where(lane_n == 127, g, roll_lanes(low, 127)))
                    down = jnp.where(lane_n == 0, cd * (g - low), roll_lanes(up, 1))
                    zf.append((down, up))
                    if not last:
                        back = roll_lanes(jnp.where(lane8 == 127, up[0:8], down[0:8]), xi * 8 + 5)
                        q_ref[8 * t : 8 * t + 8, :] = jnp.where(mine, back, q_ref[8 * t : 8 * t + 8, :])
                out = advance(values, kappa, heats, table(yz, n), (list(zip(left, right)), yf, zf))
                for m, v in enumerate(out):
                    dst[pl.ds(pl.multiple_of(xi * 512 + 16 * m, 8), n), :] = v
                return right

            def src_k(xi, n):
                return m0[pl.ds(pl.multiple_of(xi * 512 + 27 * 16, 8), n), :]

            def src_a(xi, n):
                return m0[pl.ds(pl.multiple_of(xi * 512 + 28 * 16, 8), n), :]

            left = xflux(rows_of(src, first - 1, n), rows_of(src, first, n), first - 1, n)
            if end - first == 2:
                body(first + 1, body(first, left))
            else:
                lax.fori_loop(0, (end - first) // 2, lambda t, c: body(first + 2 * t + 1, body(first + 2 * t, c)), left)

        if not last:
            n = 16 if step == 0 else 8
            hv = [v[0:n] for v in hv]
            idx_n = lane_iota(n) % 8
            xm = [xhtab[(3 * step + t) * 8 : (3 * step + t) * 8 + 8, :] for t in range(3)]
            heat = h0[28 * 16 : 28 * 16 + n, :]
            heats = [heat * wide(v, n) for v in xm]
            c = ch[0:n, :]
            xf = []
            for low, high in line_faces(hv, 9):
                up = c * (high - roll_lanes(low, 120))
                xf.append((roll_lanes(up, 8), up))
            c = ch[16 : 16 + n, :]
            yf = []
            for low, high in line_faces(hv, 3):
                up = c * (high - shift_rows(low, True))
                yf.append((shift_rows(up, False), up))
            c = ch[32 : 32 + n, :]
            zf = []
            for t, (low, high) in enumerate(line_faces(hv, 1)):
                up = c * (high - roll_lanes(low, 127))
                q = wide(q_ref[8 * t : 8 * t + 8, :], n)
                down = jnp.where(idx_n == 4, q, roll_lanes(up, 1))
                zf.append((down, jnp.where(idx_n == 3, roll_lanes(q, 126), up)))
            kappa = DT * h0[27 * 16 : 27 * 16 + n, :]
            out = advance(hv, kappa, heats, table(yzh, n), (xf, yf, zf))
            for m, v in enumerate(out):
                hdst[16 * m : 16 * m + n, :] = v
        src, dst, hsrc, hdst = dst, src, hdst, hsrc

    live = live_ref[...]
    for p in range(2):
        modes = [pair(src, p, m) for m in range(27)]
        for g, m in enumerate(LOW):
            at = 16 * g + 8 * p
            inc[at : at + 8, :] = (modes[m] - old[at : at + 8, :]) * live
        for n, v in enumerate(nodal_grid(modes)):
            t_out[n, 8 * p : 8 * p + 8, :] = v

    out_copy = pltpu.make_async_copy(t_out, t_hbm, sem)
    out_copy.start()

    ones = row_iota(16)
    for c in range(16):
        lanes = slice(128 * c, 128 * c + 128)
        v = inc[pl.ds(c, 8, stride=16), :]
        hi = v.astype(jnp.bfloat16).astype(F32)
        lo = v - hi
        owner = jnp.broadcast_to(own_ref[c : c + 1, :], (8, 128))
        picks = [owner == o for o in range(OWNERS)]
        amat[0:128, lanes] = jnp.concatenate([jnp.where(k, hi, 0.0) for k in picks], axis=0).astype(jnp.bfloat16)
        amat[128:256, lanes] = jnp.concatenate([jnp.where(k, lo, 0.0) for k in picks], axis=0).astype(jnp.bfloat16)
        owner16 = jnp.broadcast_to(own_ref[c : c + 1, :], (16, 128))
        amat[256:272, lanes] = jnp.where(owner16 == ones, wide(live, 16), 0.0).astype(jnp.bfloat16)
    total = lax.dot_general(
        amat[...], bmat[...], (((1,), (1,)), ((), ())), preferred_element_type=F32
    )
    csum[0:128, :] = (total[0:128] + total[128:256])[:, 0:128]
    csum[128:256, :] = (total[0:128] + total[128:256])[:, 128:256]
    for h in range(2):
        for g in range(8):
            pay_out[pl.ds(2 * g + h, 16, stride=18), :] = csum[pl.ds(128 * h + g, 16, stride=8), :]
        pay_out[pl.ds(16 + h, 16, stride=18), :] = total[256:272, 128 * h : 128 * h + 128]
    out_copy.wait()


def gradient_table():
    spots = [0.5 - 0.5 / math.sqrt(3.0), 0.5 + 0.5 / math.sqrt(3.0)]
    out = np.zeros((3, 8, 8), np.float32)
    for node in range(8):
        corner = [node // 4, node // 2 % 2, node % 2]
        for point in range(8):
            place = [spots[point // 4], spots[point // 2 % 2], spots[point % 2]]
            values = [place[k] if corner[k] else 1.0 - place[k] for k in range(3)]
            slopes = [1.0 if corner[k] else -1.0 for k in range(3)]
            out[0, node, point] = slopes[0] * values[1] * values[2] / 8.0
            out[1, node, point] = values[0] * slopes[1] * values[2] / 8.0
            out[2, node, point] = values[0] * values[1] * slopes[2] / 8.0
    return out


def column(values):
    rows = row_iota(8)
    out = jnp.full((8, 128), float(values[7]), F32)
    for r in range(7):
        out = jnp.where(rows == r, float(values[r]), out)
    return out


def mechanics_kernel(got_ref, de_ref, st_ref, lim_ref, stress_hbm, force_hbm, stress_out, force_out, sems):
    sums = got_ref[0:18, :]
    for s in range(1, OWNERS):
        sums = sums + got_ref[18 * s : 18 * s + 18, :]
    root = 1.0 / math.sqrt(3.0)
    rows = row_iota(8)
    signs = [jnp.where(rows // w % 2 == 0, -root, root) for w in (4, 2, 1)]
    table = gradient_table()
    cols = [[column(table[d, :, g]) for g in range(8)] for d in range(3)]
    for h in range(2):
        lanes = slice(128 * h, 128 * h + 128)
        inv = 1.0 / jnp.maximum(sums[16 + h : 17 + h], 1.0)

        def row(m):
            return jnp.broadcast_to(sums[2 * m + h : 2 * m + h + 1] * inv, (8, 128))

        z = [row(2 * n) + signs[2] * row(2 * n + 1) for n in range(4)]
        y = [z[2 * n] + signs[1] * z[2 * n + 1] for n in range(2)]
        strain = EXPANSION * (y[0] + signs[0] * y[1])
        normal = [de_ref[k, :, lanes] - strain for k in range(3)]
        volume = normal[0] + normal[1] + normal[2]
        trial = [st_ref[k, :, lanes] + LAME * volume + 2.0 * MU * normal[k] for k in range(3)]
        shear = [st_ref[k, :, lanes] + 2.0 * MU * de_ref[k, :, lanes] for k in range(3, 6)]
        pressure = (trial[0] + trial[1] + trial[2]) * (1.0 / 3.0)
        dev = [t - pressure for t in trial]
        squares = dev[0] * dev[0] + dev[1] * dev[1] + dev[2] * dev[2]
        squares = squares + 2.0 * (shear[0] * shear[0] + shear[1] * shear[1] + shear[2] * shear[2])
        equivalent = jnp.sqrt(1.5 * squares)
        limit = jnp.broadcast_to(lim_ref[0:1, lanes], (8, 128))
        plastic = jnp.maximum(equivalent - limit, 0.0) * (1.0 / (3.0 * MU + HARD))
        factor = 1.0 - (3.0 * MU) * plastic / jnp.maximum(equivalent, limit)
        stress = [pressure + factor * d for d in dev] + [factor * s for s in shear]
        for k in range(6):
            stress_out[k, :, lanes] = stress[k]
        index = [[0, 5, 4], [5, 1, 3], [4, 3, 2]]
        forces = [jnp.zeros((8, 128), F32)] * 3
        for g in range(8):
            at = [jnp.broadcast_to(s[g : g + 1], (8, 128)) for s in stress]
            for c in range(3):
                for d in range(3):
                    forces[c] = forces[c] + cols[d][g] * at[index[c][d]]
        for c in range(3):
            force_out[c, :, lanes] = forces[c]
    fetch(((stress_out, stress_hbm), (force_out, force_hbm)), sems)


def swap(first, second, axis, count):
    even = [(i, i ^ 1) for i in range(count)]
    odd = [(i, i + 1 if i % 2 else i - 1) for i in range(1, count - 1)]
    a = lax.ppermute(first, axis, even)
    b = lax.ppermute(second, axis, odd)
    return a, b


def program(temps, cond, absorb, layers, owner, cell, de, st, lim):
    vm = lambda n: pltpu.VMEM((n, 128), F32)
    sx, sy, sz = (lax.axis_size(a) for a in ("gx", "gy", "gz"))
    cols, zpay, live = call(
        prep_kernel,
        (vm(512), vm(32), vm(8)),
        (temps.reshape(27, 16, 128), cond.reshape(16, 128), absorb.reshape(16, 128), layers),
        scratch=[
            pltpu.VMEM((27, 16, 128), F32), vm(16), vm(16), pltpu.SemaphoreType.DMA((3,)),
        ],
        far=(0, 1, 2, 3),
    )
    za, zb = swap(zpay, zpay, "gz", sz)
    xf, xs, hown = call(xpay_kernel, (vm(XROWS), vm(XROWS), vm(32)), (cols, za, zb))
    xa, xb = swap(xf, xs, "gx", sx)
    yf, ys = call(ypay_kernel, (vm(YROWS), vm(YROWS)), (cols, xa, xb, hown))
    ya, yb = swap(yf, ys, "gy", sy)
    m0, h0, yz, yzh, xtab, xhtab, old, bmat, own = call(
        pre_kernel,
        (
            vm(6144), vm(512), vm(144), vm(144), vm(192), vm(96), vm(128),
            pltpu.VMEM((256, 2048), jnp.bfloat16), pltpu.VMEM((16, 128), jnp.int32),
        ),
        (cols, hown, xa, xb, owner.reshape(16, 128), cell.reshape(16, 128)),
        scratch=[pltpu.VMEM((16, 128), jnp.int32), pltpu.SemaphoreType.DMA((2,))],
        far=(4, 5),
    )
    t_new, pay, _, _ = call(
        main_kernel,
        (pltpu.HBM((27, 16, 128), F32), vm(OWNERS * 18), vm(6144), vm(512)),
        (m0, h0, yz, yzh, xtab, xhtab, old, bmat, xa, xb, ya, yb, hown, own, live),
        scratch=[
            pltpu.VMEM((27, 16, 128), F32), pltpu.SemaphoreType.DMA, vm(6144), vm(512), vm(192), vm(192), vm(192), vm(192), vm(48), vm(144), vm(72), vm(128),
            pltpu.VMEM((272, 2048), jnp.bfloat16), vm(256),
        ],
        aliases={0: 2, 1: 3},
    )
    got = lax.all_to_all(pay.reshape(OWNERS, 1, 2304), "gx", 0, 0, tiled=True)
    stress, forces = call(
        mechanics_kernel,
        (pltpu.HBM((6, 8, 256), F32), pltpu.HBM((3, 8, 256), F32)),
        (got.reshape(OWNERS * 18, 128), de, st, lim.reshape(1, 256)),
        scratch=[pltpu.VMEM((6, 8, 256), F32), pltpu.VMEM((3, 8, 256), F32), pltpu.SemaphoreType.DMA((2,))],
    )
    return t_new.reshape(3, 3, 3, 4, 4, 128), stress, forces


def solution(mesh):
    cells = P(None, None, ("gx", "gy", "gz"))
    temps = P(None, None, None, "gx", "gy", "gz")
    block = P("gx", "gy", "gz")
    return jax.shard_map(
        program,
        mesh=mesh,
        in_specs=(
            temps, block, block, block, P("gx", "gy", "gz", None, None), P("gx", "gy", "gz", None),
            cells, cells, P(("gx", "gy", "gz")),
        ),
        out_specs=(temps, cells, cells),
        check_vma=False,
    )
```

```python
import functools
import math

import jax
import jax.numpy as jnp
import numpy as np
from jax import lax
from jax.experimental import pallas as pl
from jax.experimental.pallas import tpu as pltpu
from jax.sharding import PartitionSpec as P


STEPS = 4
DT = 0.003
PENALTY = 3.0
HEAT = 100.0 * (2.0 / 3.0)
EXPANSION = 0.02
MU = 100.0 / 2.6
LAME = 30.0 / 0.52
HARD = 10.0
NX, NY, NZ = 64, 32, 512
PX, PY, PZ = 4, 4, 128
OWNERS, CELLS = 16, 256
FIRST = 8
F32 = jnp.float32

LAM = (0.0, 12.0, 24.0)
ROWS = 29

XFULL = {(d, y): ((d - 1) * 4 + y) * ROWS for d in (1, 2, 3) for y in range(4)}
XFACE = [12 * ROWS + 10 * y for y in range(4)]
XH = 12 * ROWS + 40
XROWS = 424
YFULL = {(d, x): ((d - 1) * 4 + x) * ROWS for d in (1, 2, 3) for x in range(4)}
YFACE = [12 * ROWS + 10 * x for x in range(4)]
NEAR = [(side, xd, d) for side in (0, 1) for xd in (1, 2) for d in range(1, 4 - xd)]
EDGE = [(side, xd, 4 - xd) for side in (0, 1) for xd in (1, 2, 3)]
YNEAR = [12 * ROWS + 40 + ROWS * n for n in range(6)]
YEDGE = [18 * ROWS + 40 + 16 * n for n in range(6)]
YH = [18 * ROWS + 136, 19 * ROWS + 136]
YROWS = 720


def mode(i, j, l):
    return 9 * i + 3 * j + l


def call(kernel, outs, args, scratch=(), far=(), aliases=None):
    def place(n, a):
        return a if a.size == 1 else pltpu.with_memory_space_constraint(a, pltpu.HBM if n in far else pltpu.VMEM)

    return pl.pallas_call(
        kernel,
        out_shape=outs,
        in_specs=[
            pl.BlockSpec(memory_space=pltpu.SMEM if a.size == 1 else pltpu.HBM if n in far else pltpu.VMEM)
            for n, a in enumerate(args)
        ],
        out_specs=tuple(pl.BlockSpec(memory_space=o.memory_space) for o in outs),
        input_output_aliases=aliases or {},
        compiler_params=pltpu.CompilerParams(vmem_limit_bytes=24 << 20),
        scratch_shapes=list(scratch),
    )(*[place(n, a) for n, a in enumerate(args)])


def fetch(pairs, sems):
    copies = [pltpu.make_async_copy(a, b, sems.at[n]) for n, (a, b) in enumerate(pairs)]
    for c in copies:
        c.start()
    for c in copies:
        c.wait()


def lane_iota(rows):
    return lax.broadcasted_iota(jnp.int32, (rows, 128), 1)


def row_iota(rows):
    return lax.broadcasted_iota(jnp.int32, (rows, 128), 0)


def modal(a, b, c):
    s = a + c
    return (s + 4.0 * b) * (1.0 / 6.0), (c - a) * 0.5, (s - 2.0 * b) * (1.0 / 3.0)


def modal_grid(values):
    for stride in (9, 3, 1):
        out = [None] * 27
        for base in range(27):
            if base // stride % 3 == 0:
                ids = [base + stride * t for t in range(3)]
                for q, r in zip(ids, modal(*[values[q] for q in ids])):
                    out[q] = r
        values = out
    return values


def nodal_grid(values):
    for stride in (9, 3, 1):
        out = [None] * 27
        for base in range(27):
            if base // stride % 3 == 0:
                al, be, ga = (values[base + stride * t] for t in range(3))
                e = al + ga
                out[base], out[base + stride], out[base + 2 * stride] = e - be, al - 0.5 * ga, e + be
        values = out
    return values


def prep_kernel(t_in, k_in, a_in, lay_ref, cols_ref, zpay_ref, live_ref, t_ref, k_ref, a_ref, sems):
    fetch(((t_in, t_ref), (k_in, k_ref), (a_in, a_ref)), sems)
    m = (lane_iota(8) < lay_ref[0, 0, 0]).astype(F32)
    live_ref[...] = m
    lane = lane_iota(32)
    for h in range(2):
        rows = slice(8 * h, 8 * h + 8)
        modes = modal_grid([t_ref[n, rows, :] for n in range(27)])
        modes.append(k_ref[rows, :] * m)
        modes.append(a_ref[rows, :] * m * (DT * HEAT))
        for n, v in enumerate(modes):
            cols_ref[pl.ds(8 * h * 32 + n, 8, stride=32), :] = v
    zero = jnp.zeros((3, 128), F32)
    acc = jnp.zeros((32, 128), F32)
    for c in range(16):
        cols_ref[c * 32 + 29 : c * 32 + 32, :] = zero
    for c in range(16):
        x, y = c // 4, c % 4
        start = y * 32 + x * 8
        v = pltpu.roll(cols_ref[c * 32 : c * 32 + 32, :], (4 + start) % 128, axis=1)
        acc = jnp.where((lane >= start) & (lane < start + 8), v, acc)
    zpay_ref[...] = acc


def upper_first(axis):
    at = lax.axis_index(axis)
    return (at + lax.axis_index("gy") if axis == "gx" else at) % 2 == 0


def by_parity(axis, write, first, second):
    even = upper_first(axis)

    @pl.when(even)
    def _():
        write(first, second)

    @pl.when(jnp.logical_not(even))
    def _():
        write(second, first)


def face_rows(cols_ref, c, axis, sign):
    base = c * 32
    if axis == 0:
        parts = [cols_ref[base + 9 * i : base + 9 * i + 9, :] for i in range(3)]
        return [parts[0] + parts[2] + sign * parts[1]]
    out = []
    for i in range(3):
        parts = [cols_ref[base + 9 * i + 3 * j : base + 9 * i + 3 * j + 3, :] for j in range(3)]
        out.append(parts[0] + parts[2] + sign * parts[1])
    return out


def put_faces(dst, at, cols_ref, c, axis, sign):
    row = at
    for part in face_rows(cols_ref, c, axis, sign):
        dst[row : row + part.shape[0], :] = part
        row += part.shape[0]
    dst[row : row + 1, :] = cols_ref[c * 32 + 27 : c * 32 + 28, :]


def xhalo_block(even, xa_ref, xb_ref, side, at, rows):
    a, b = xa_ref[at : at + rows, :], xb_ref[at : at + rows, :]
    return jnp.where(even, b, a) if side == 0 else jnp.where(even, a, b)


def xpay_kernel(cols_ref, za_ref, zb_ref, first_ref, second_ref, h_ref):
    even = upper_first("gz")
    idx = lane_iota(32) % 8
    za, zb = za_ref[...], zb_ref[...]
    upper = jnp.where(even, za, zb)
    lower = jnp.where(even, zb, za)
    own = jnp.where(idx < 4, lower, upper)
    h_ref[...] = own

    def write(upper_ref, lower_ref):
        for (d, y), at in XFULL.items():
            up, down = ((4 - d) * 4 + y) * 32, ((d - 1) * 4 + y) * 32
            upper_ref[at : at + ROWS, :] = cols_ref[up : up + ROWS, :]
            lower_ref[at : at + ROWS, :] = cols_ref[down : down + ROWS, :]
        for y in range(4):
            put_faces(upper_ref, XFACE[y], cols_ref, y, 0, 1.0)
            put_faces(lower_ref, XFACE[y], cols_ref, 12 + y, 0, -1.0)
        for ref in (upper_ref, lower_ref):
            ref[XH : XH + ROWS, :] = own[0:ROWS]

    by_parity("gx", write, first_ref, second_ref)


def ypay_kernel(cols_ref, xa_ref, xb_ref, h_ref, first_ref, second_ref):
    halo = functools.partial(xhalo_block, upper_first("gx"), xa_ref, xb_ref)

    def corner(side, at, ysign):
        xsign = 1.0 if side == 0 else -1.0
        c = [halo(side, at + 9 * i, 9) for i in range(3)]
        xface = c[0] + c[2] + xsign * c[1]
        yface = [v[0:3] + v[6:9] + ysign * v[3:6] for v in c[1:]]
        return (xface[0:3] - xsign * yface[0] - yface[1], xface[3:9], yface[0], yface[1], halo(side, at + 27, 1))

    def write(upper_ref, lower_ref):
        for (d, x), at in YFULL.items():
            up, down = (x * 4 + 4 - d) * 32, (x * 4 + d - 1) * 32
            upper_ref[at : at + ROWS, :] = cols_ref[up : up + ROWS, :]
            lower_ref[at : at + ROWS, :] = cols_ref[down : down + ROWS, :]
        for x in range(4):
            put_faces(upper_ref, YFACE[x], cols_ref, x * 4, 1, 1.0)
            put_faces(lower_ref, YFACE[x], cols_ref, x * 4 + 3, 1, -1.0)
        for (side, xd, d), at in zip(NEAR, YNEAR):
            upper_ref[at : at + ROWS, :] = halo(side, XFULL[xd, 4 - d], ROWS)
            lower_ref[at : at + ROWS, :] = halo(side, XFULL[xd, d - 1], ROWS)
        for (side, xd, d), at in zip(EDGE, YEDGE):
            for ref, y, sign in ((upper_ref, 4 - d, 1.0), (lower_ref, d - 1, -1.0)):
                row = at
                for part in corner(side, XFULL[xd, y], sign):
                    ref[row : row + part.shape[0], :] = part
                    row += part.shape[0]
        beside = jnp.where(lane_iota(ROWS) // 8 % 4 < 2, halo(1, XH, ROWS), halo(0, XH, ROWS))
        for ref in (upper_ref, lower_ref):
            ref[YH[0] : YH[0] + ROWS, :] = h_ref[0:ROWS, :]
            ref[YH[1] : YH[1] + ROWS, :] = beside

    by_parity("gy", write, first_ref, second_ref)


def couple(k1, k2):
    return (2.0 * PENALTY * DT) * k1 * k2 / jnp.maximum(k1 + k2, 1.0)


def roll_lanes(v, shift):
    return pltpu.roll(v, shift, axis=1)


def wide(v, n):
    return v if n == 8 else jnp.concatenate([v, v], axis=0)


def shift_rows(v, up):
    n = v.shape[0]
    amount, edge = (7, 7) if up else (1, 0)
    if n == 8:
        return pltpu.roll(v, amount, axis=0)
    a, b = pltpu.roll(v[0:8], amount, axis=0), pltpu.roll(v[8:16], amount, axis=0)
    take = row_iota(8) == edge
    return jnp.concatenate([jnp.where(take, b, a), jnp.where(take, a, b)], axis=0)


def line_faces(values, stride):
    out = []
    for base in range(27):
        if base // stride % 3 == 0:
            e = values[base] + values[base + 2 * stride]
            out.append((e - values[base + stride], e + values[base + stride]))
    return out


def bounded(inner, outer, c, c_outer):
    rows = row_iota(8)
    top, bottom = rows == 7, rows == 0
    turn = jnp.where(bottom, -1.0, 1.0)
    c_below = pltpu.roll(c_outer, 1, axis=0)
    out = []
    for n, (low, high) in enumerate(line_faces(inner, 3)):
        base = n // 3 * 9 + n % 3
        beside = outer[base] + outer[base + 6] + turn * outer[base + 3]
        up = c * (high - jnp.where(top, pltpu.roll(beside, 7, axis=0), pltpu.roll(low, 7, axis=0)))
        down = jnp.where(bottom, c_below * (pltpu.roll(beside, 1, axis=0) - low), pltpu.roll(up, 1, axis=0))
        out.append((down, up))
    return out


def slot(y):
    return (y + 2) % 16


def advance(values, kappa, heats, yz, fluxes):
    factor = {}
    for total in sorted({LAM[i] + LAM[j] + LAM[l] for i in range(3) for j in range(3) for l in range(3)}):
        factor[total] = 1.0 - kappa * total if total else None
    terms = []
    for lines in fluxes:
        per = []
        for low, high in lines:
            gain, both = low - high, low + high
            per.append((gain, -3.0 * both, 2.0 * gain))
        terms.append(per)
    out = []
    for i in range(3):
        for j in range(3):
            for l in range(3):
                v = values[mode(i, j, l)]
                f = factor[LAM[i] + LAM[j] + LAM[l]]
                v = v if f is None else v * f
                v = v + heats[i] * yz[3 * j + l]
                v = v + (terms[0][3 * j + l][i] + terms[1][3 * i + l][j]) + terms[2][3 * i + j][l]
                out.append(v)
    return out


def gauss_exp(offset, near, far):
    scaled = offset * jnp.where(offset >= 0.0, 1.0 / near, 1.0 / far)
    return jnp.exp(-3.0 * (scaled * scaled))


def place(m0, x, y, block):
    m0[pl.ds((x + 4) * 512 + slot(y), ROWS, stride=16), :] = block


def place_h(h0, row, y, blocks):
    lane = lane_iota(ROWS)
    rolled = [roll_lanes(b, (32 * n - 32 * y) % 128) if (n - y) % 4 else b for n, b in enumerate(blocks)]
    v = jnp.where(lane < 32, rolled[0], jnp.where(lane < 64, rolled[1], rolled[2]))
    h0[pl.ds(row, ROWS, stride=16), :] = jnp.where(lane < 96, v, 0.0)


def pair(ref, p, m):
    a = ref[pl.ds((4 + 2 * p) * 512 + 16 * m, 8), :]
    b = ref[pl.ds((5 + 2 * p) * 512 + 16 * m, 8), :]
    return jnp.where(row_iota(8) < 4, pltpu.roll(a, 6, axis=0), pltpu.roll(b, 2, axis=0))


LOW = [mode(i, j, l) for i in range(2) for j in range(2) for l in range(2)]


def line_modes(base, centre, near, far):
    return modal(*[gauss_exp(base + 0.5 * n - centre, near, far) for n in range(3)])


def pre_kernel(
    cols_ref, h_ref, xa_ref, xb_ref, own_in, cell_in,
    m0, h0, yz, yzh, xtab, xhtab, old, bmat, own_out,
    cell_ref, sems,
):
    gx, gy, gz = lax.axis_index("gx"), lax.axis_index("gy"), lax.axis_index("gz")
    even_x = upper_first("gx")
    fetch(((own_in, own_out), (cell_in, cell_ref)), sems)

    def clear(n, _):
        m0[pl.ds(pl.multiple_of(n * 128, 128), 128), :] = jnp.zeros((128, 128), F32)
        return 0

    lax.fori_loop(0, 48, clear, 0)
    h0[...] = jnp.zeros((512, 128), F32)
    xhalo = functools.partial(xhalo_block, even_x, xa_ref, xb_ref)
    for c in range(16):
        place(m0, c // 4, c % 4, cols_ref[c * 32 : c * 32 + ROWS, :])
    for side in (0, 1):
        for d in range(1, 4):
            x = -d if side == 0 else 3 + d
            for y in range(4):
                place(m0, x, y, xhalo(side, XFULL[d, y], ROWS))
        x = -4 if side == 0 else 7
        for y in range(4):
            block = xhalo(side, XFACE[y], 10)
            at = (x + 4) * 512 + slot(y)
            m0[pl.ds(at, 8, stride=16), :] = block[0:8]
            m0[pl.ds(at + 8 * 16, 1), :] = block[8:9]
            m0[pl.ds(at + 27 * 16, 1), :] = block[9:10]
    blocks = [xhalo(0, XH, ROWS), h_ref[0:ROWS, :], xhalo(1, XH, ROWS)]
    for y in range(4):
        place_h(h0, slot(y), y, blocks)

    lane16 = lane_iota(16)
    idx16 = lane16 % 8
    s16 = row_iota(16)
    ypos = (gy * PY + jnp.where(s16 < 12, s16 - 2, s16 - 18)).astype(F32)
    ymodes = line_modes(ypos, NY * 0.5, NY / 4.0, NY / 4.0)
    zpos = (gz * PZ + lane16).astype(F32)
    zmodes = line_modes(zpos, NZ * 0.75, NZ / 8.0, NZ / 8.0)
    zhpos = (gz * PZ + jnp.where(idx16 < 4, idx16 - 4, idx16 + 124)).astype(F32)
    zhmodes = line_modes(zhpos, NZ * 0.75, NZ / 8.0, NZ / 8.0)
    for j in range(3):
        for l in range(3):
            at = (3 * j + l) * 16
            yz[at : at + 16, :] = ymodes[j] * zmodes[l]
            yzh[at : at + 16, :] = ymodes[j] * zhmodes[l]
    for step in range(STEPS):
        centre = NX * 0.5 + step * NX / 16.0
        for t, v in enumerate(line_modes((gx * PX + s16 - 4).astype(F32), centre, NX / 8.0, NX / 4.0)):
            xtab[(3 * step + t) * 16 : (3 * step + t) * 16 + 16, :] = v
        for t, v in enumerate(line_modes((gx * PX + lane_iota(8) // 8 - 4).astype(F32), centre, NX / 8.0, NX / 4.0)):
            xhtab[(3 * step + t) * 8 : (3 * step + t) * 8 + 8, :] = v

    for g, m in enumerate(LOW):
        for p in range(2):
            old[16 * g + 8 * p : 16 * g + 8 * p + 8, :] = pair(m0, p, m)
    for c in range(16):
        cell = jnp.broadcast_to(cell_ref[c : c + 1, :], (CELLS, 128))
        hit = cell == row_iota(CELLS)
        bmat[:, 128 * c : 128 * c + 128] = jnp.where(hit, 1.0, 0.0).astype(jnp.bfloat16)


def main_kernel(
    m0_in, h0_in, yz, yzh, xtab, xhtab, old, bmat, xa_ref, xb_ref, ya_ref, yb_ref, h_ref, own_ref, live_ref,
    t_hbm, pay_out, m0, h0,
    t_out, sem, m1, h1, cx, cy, czu, czd, ch, gs, q_ref, inc, amat, csum,
):
    del m0_in, h0_in
    even_y = upper_first("gy")
    lane8 = lane_iota(8)
    zeros8 = jnp.zeros((8, 128), F32)

    def yhalo(side, at, rows):
        a, b = ya_ref[at : at + rows, :], yb_ref[at : at + rows, :]
        return jnp.where(even_y, b, a) if side == 0 else jnp.where(even_y, a, b)

    for side in (0, 1):
        out = [-d if side == 0 else 3 + d for d in range(5)]
        for (d, x), at in YFULL.items():
            place(m0, x, out[d], yhalo(side, at, ROWS))
        for x in range(4):
            block = yhalo(side, YFACE[x], 10)
            at = (x + 4) * 512 + slot(out[4])
            for i in range(3):
                for l in range(3):
                    m0[pl.ds(at + mode(i, 0, l) * 16, 1), :] = block[3 * i + l : 3 * i + l + 1]
            m0[pl.ds(at + 27 * 16, 1), :] = block[9:10]
        for (xside, xd, d), at in zip(NEAR, YNEAR):
            place(m0, -xd if xside == 0 else 3 + xd, out[d], yhalo(side, at, ROWS))
        for (xside, xd, d), at in zip(EDGE, YEDGE):
            block = yhalo(side, at, 16)
            to = ((-xd if xside == 0 else 3 + xd) + 4) * 512 + slot(out[d])
            m0[pl.ds(to, 8, stride=16), :] = block[0:8]
            for row, m in enumerate((8, 9, 10, 11, 18, 19, 20, 27), 8):
                m0[pl.ds(to + 16 * m, 1), :] = block[row : row + 1]
        beside = yhalo(side, YH[1], ROWS)
        blocks = [beside, yhalo(side, YH[0], ROWS), beside]
        for y in range(4):
            place_h(h0, slot(8 * side - 4 + y), y, blocks)

    lane16 = lane_iota(16)
    idx16 = lane16 % 8
    kh = h0[27 * 16 : 28 * 16, :]
    gk_src = jnp.where(idx16 == 5, roll_lanes(kh, 2), kh)
    ch[0:16, :] = couple(kh, roll_lanes(kh, 120))
    ch[16:32, :] = couple(kh, shift_rows(kh, True))
    ch[32:48, :] = jnp.where((idx16 == 3) | (idx16 == 7), 0.0, couple(kh, roll_lanes(kh, 127)))

    def kof(xi, n):
        return m0[xi * 512 + 27 * 16 : xi * 512 + 27 * 16 + n, :]

    for xi in range(11):
        n = 16 if 2 <= xi < 9 else 8
        at = slice(xi * 16, xi * 16 + n)
        k = kof(xi, n)
        cx[at, :] = couple(k, kof(xi + 1, n))
        if xi == 0:
            continue
        gk = roll_lanes(gk_src[0:n], (123 - xi * 8) % 128)
        cy[at, :] = couple(k, shift_rows(k, True))
        czu[at, :] = couple(k, jnp.where(lane_iota(n) == 127, gk, roll_lanes(k, 127)))
        czd[at, :] = couple(k, gk)

    def rows_of(ref, xi, n):
        return [ref[pl.ds(pl.multiple_of(xi * 512 + 16 * m, 8), n), :] for m in range(27)]

    def at_x(ref, xi, n):
        return ref[pl.ds(pl.multiple_of(xi * 16, 8), n), :]

    def table(ref, n):
        return [ref[16 * t : 16 * t + n, :] for t in range(9)]

    groups = [
        [(1, 3, 8, False), (3, 4, 8, True), (4, 8, 16, False), (8, 9, 8, True), (9, 11, 8, False)],
        [(2, 4, 8, False), (4, 8, 8, True), (8, 10, 8, False)],
        [(3, 9, 8, False)],
        [(4, 6, 8, False), (6, 8, 8, False)],
    ]
    live = live_ref[...]
    out_copies = [
        pltpu.make_async_copy(t_out.at[:, 8 * p : 8 * p + 8, :], t_hbm.at[:, 8 * p : 8 * p + 8, :], sem.at[p])
        for p in range(2)
    ]

    def finish(ref, p):
        modes = [pair(ref, p, m) for m in range(27)]
        for n, v in enumerate(nodal_grid(modes)):
            t_out[n, 8 * p : 8 * p + 8, :] = v
        out_copies[p].start()
        for g, m in enumerate(LOW):
            at = 16 * g + 8 * p
            inc[at : at + 8, :] = (modes[m] - old[at : at + 8, :]) * live

    src, dst, hsrc, hdst = m0, m1, h0, h1
    for step in range(STEPS):
        last = step == STEPS - 1
        hn = 16 if step == 0 else 8
        hv = [hsrc[16 * m : 16 * m + hn, :] for m in range(27)]
        lane_h = lane_iota(hn)
        idx_h = lane_h % 8
        hz = line_faces(hv, 1)
        for t, (low, high) in enumerate(hz):
            gs[16 * t : 16 * t + hn, :] = jnp.where(idx_h == 5, roll_lanes(high, 2), low)
        if not last:
            for t in range(9):
                q_ref[8 * t : 8 * t + 8, :] = zeros8

        for first, end, n, beyond in groups[step]:
            lane_n = lane_iota(n)

            def xflux(here, there, xi, n=n):
                c = at_x(cx, xi, n)
                return tuple(c * (a[1] - b[0]) for a, b in zip(line_faces(here, 9), line_faces(there, 9)))

            def body(xi, carry, n=n, src=src, dst=dst, step=step, last=last, lane_n=lane_n, beyond=beyond):
                left = carry
                values = rows_of(src, xi, n)
                following = rows_of(src, xi + 1, n)
                right = xflux(values, following, xi, n)
                kappa = DT * src_k(xi, n)
                heat = src_a(xi, n)
                xm = [xtab[pl.ds((3 * step + t) * 16 + xi, 1), :] for t in range(3)]
                heats = [heat * jnp.broadcast_to(v, (n, 128)) for v in xm]
                c = at_x(cy, xi, n)
                if beyond:
                    outer = [src[pl.ds(pl.multiple_of(xi * 512 + 16 * m + 8, 8), 8), :] for m in range(27)]
                    yf = bounded(values, outer, c, cy[pl.ds(pl.multiple_of(xi * 16 + 8, 8), 8), :])
                else:
                    yf = []
                    for low, high in line_faces(values, 3):
                        up = c * (high - shift_rows(low, True))
                        yf.append((shift_rows(up, False), up))
                cu, cd = at_x(czu, xi, n), at_x(czd, xi, n)
                zf = []
                shift = 123 - xi * 8
                mine = (lane8 == xi * 8 + 4) | (lane8 == xi * 8 + 5)
                for t, (low, high) in enumerate(line_faces(values, 1)):
                    g = roll_lanes(gs[16 * t : 16 * t + n, :], shift)
                    up = cu * (high - jnp.where(lane_n == 127, g, roll_lanes(low, 127)))
                    down = jnp.where(lane_n == 0, cd * (g - low), roll_lanes(up, 1))
                    zf.append((down, up))
                    if not last:
                        back = roll_lanes(jnp.where(lane8 == 127, up[0:8], down[0:8]), xi * 8 + 5)
                        q_ref[8 * t : 8 * t + 8, :] = jnp.where(mine, back, q_ref[8 * t : 8 * t + 8, :])
                out = advance(values, kappa, heats, table(yz, n), (list(zip(left, right)), yf, zf))
                for m, v in enumerate(out):
                    dst[pl.ds(pl.multiple_of(xi * 512 + 16 * m, 8), n), :] = v
                return right

            def src_k(xi, n):
                return m0[pl.ds(pl.multiple_of(xi * 512 + 27 * 16, 8), n), :]

            def src_a(xi, n):
                return m0[pl.ds(pl.multiple_of(xi * 512 + 28 * 16, 8), n), :]

            left = xflux(rows_of(src, first - 1, n), rows_of(src, first, n), first - 1, n)
            if end - first <= 2:
                for xi in range(first, end):
                    left = body(xi, left)
                if last:
                    finish(dst, first // 2 - 2)
            else:
                lax.fori_loop(0, (end - first) // 2, lambda t, c: body(first + 2 * t + 1, body(first + 2 * t, c)), left)

        if not last:
            n = 8
            inner = [v[0:8] for v in hv]
            idx_n = lane_iota(n) % 8
            xm = [xhtab[(3 * step + t) * 8 : (3 * step + t) * 8 + 8, :] for t in range(3)]
            heat = h0[28 * 16 : 28 * 16 + n, :]
            heats = [heat * wide(v, n) for v in xm]
            c = ch[0:n, :]
            xf = []
            for low, high in line_faces(inner, 9):
                up = c * (high - roll_lanes(low, 120))
                xf.append((roll_lanes(up, 8), up))
            c = ch[16 : 16 + n, :]
            if step == 0:
                yf = bounded(inner, [v[8:16] for v in hv], c, ch[24:32, :])
            else:
                yf = []
                for low, high in line_faces(inner, 3):
                    up = c * (high - shift_rows(low, True))
                    yf.append((shift_rows(up, False), up))
            c = ch[32 : 32 + n, :]
            zf = []
            for t, (low, high) in enumerate(line_faces(inner, 1)):
                up = c * (high - roll_lanes(low, 127))
                q = wide(q_ref[8 * t : 8 * t + 8, :], n)
                down = jnp.where(idx_n == 4, q, roll_lanes(up, 1))
                zf.append((down, jnp.where(idx_n == 3, roll_lanes(q, 126), up)))
            kappa = DT * h0[27 * 16 : 27 * 16 + n, :]
            out = advance(inner, kappa, heats, table(yzh, n), (xf, yf, zf))
            for m, v in enumerate(out):
                hdst[16 * m : 16 * m + n, :] = v
        src, dst, hsrc, hdst = dst, src, hdst, hsrc

    slots = (row_iota(16) + FIRST) % OWNERS
    for c in range(16):
        lanes = slice(128 * c, 128 * c + 128)
        v = inc[pl.ds(c, 8, stride=16), :]
        hi = v.astype(jnp.bfloat16).astype(F32)
        lo = v - hi
        owner = jnp.broadcast_to(own_ref[c : c + 1, :], (8, 128))
        picks = [owner == (o + FIRST) % OWNERS for o in range(OWNERS)]
        amat[0:128, lanes] = jnp.concatenate([jnp.where(k, hi, 0.0) for k in picks], axis=0).astype(jnp.bfloat16)
        amat[128:256, lanes] = jnp.concatenate([jnp.where(k, lo, 0.0) for k in picks], axis=0).astype(jnp.bfloat16)
        owner16 = jnp.broadcast_to(own_ref[c : c + 1, :], (16, 128))
        amat[256:272, lanes] = jnp.where(owner16 == slots, wide(live, 16), 0.0).astype(jnp.bfloat16)
    total = lax.dot_general(
        amat[...], bmat[...], (((1,), (1,)), ((), ())), preferred_element_type=F32
    )
    csum[0:128, :] = (total[0:128] + total[128:256])[:, 0:128]
    csum[128:256, :] = (total[0:128] + total[128:256])[:, 128:256]
    for h in range(2):
        for g in range(8):
            pay_out[pl.ds(2 * g + h, 16, stride=18), :] = csum[pl.ds(128 * h + g, 16, stride=8), :]
        pay_out[pl.ds(16 + h, 16, stride=18), :] = total[256:272, 128 * h : 128 * h + 128]
    for c in out_copies:
        c.wait()


def gradient_table():
    spots = [0.5 - 0.5 / math.sqrt(3.0), 0.5 + 0.5 / math.sqrt(3.0)]
    out = np.zeros((3, 8, 8), np.float32)
    for node in range(8):
        corner = [node // 4, node // 2 % 2, node % 2]
        for point in range(8):
            place = [spots[point // 4], spots[point // 2 % 2], spots[point % 2]]
            values = [place[k] if corner[k] else 1.0 - place[k] for k in range(3)]
            slopes = [1.0 if corner[k] else -1.0 for k in range(3)]
            out[0, node, point] = slopes[0] * values[1] * values[2] / 8.0
            out[1, node, point] = values[0] * slopes[1] * values[2] / 8.0
            out[2, node, point] = values[0] * values[1] * slopes[2] / 8.0
    return out


def column(values):
    rows = row_iota(8)
    out = jnp.full((8, 128), float(values[7]), F32)
    for r in range(7):
        out = jnp.where(rows == r, float(values[r]), out)
    return out


def mechanics_kernel(got_ref, de_ref, st_ref, lim_ref, stress_hbm, force_hbm, stress_out, force_out, sems):
    sums = got_ref[0:18, :]
    for s in range(1, OWNERS):
        sums = sums + got_ref[18 * s : 18 * s + 18, :]
    root = 1.0 / math.sqrt(3.0)
    rows = row_iota(8)
    signs = [jnp.where(rows // w % 2 == 0, -root, root) for w in (4, 2, 1)]
    table = gradient_table()
    cols = [[column(table[d, :, g]) for g in range(8)] for d in range(3)]
    for h in range(2):
        lanes = slice(128 * h, 128 * h + 128)
        inv = 1.0 / jnp.maximum(sums[16 + h : 17 + h], 1.0)

        def row(m):
            return jnp.broadcast_to(sums[2 * m + h : 2 * m + h + 1] * inv, (8, 128))

        z = [row(2 * n) + signs[2] * row(2 * n + 1) for n in range(4)]
        y = [z[2 * n] + signs[1] * z[2 * n + 1] for n in range(2)]
        strain = EXPANSION * (y[0] + signs[0] * y[1])
        normal = [de_ref[k, :, lanes] - strain for k in range(3)]
        volume = normal[0] + normal[1] + normal[2]
        trial = [st_ref[k, :, lanes] + LAME * volume + 2.0 * MU * normal[k] for k in range(3)]
        shear = [st_ref[k, :, lanes] + 2.0 * MU * de_ref[k, :, lanes] for k in range(3, 6)]
        pressure = (trial[0] + trial[1] + trial[2]) * (1.0 / 3.0)
        dev = [t - pressure for t in trial]
        squares = dev[0] * dev[0] + dev[1] * dev[1] + dev[2] * dev[2]
        squares = squares + 2.0 * (shear[0] * shear[0] + shear[1] * shear[1] + shear[2] * shear[2])
        equivalent = jnp.sqrt(1.5 * squares)
        limit = jnp.broadcast_to(lim_ref[0:1, lanes], (8, 128))
        plastic = jnp.maximum(equivalent - limit, 0.0) * (1.0 / (3.0 * MU + HARD))
        factor = 1.0 - (3.0 * MU) * plastic / jnp.maximum(equivalent, limit)
        stress = [pressure + factor * d for d in dev] + [factor * s for s in shear]
        for k in range(6):
            stress_out[k, :, lanes] = stress[k]
        index = [[0, 5, 4], [5, 1, 3], [4, 3, 2]]
        forces = [jnp.zeros((8, 128), F32)] * 3
        for g in range(8):
            at = [jnp.broadcast_to(s[g : g + 1], (8, 128)) for s in stress]
            for c in range(3):
                for d in range(3):
                    forces[c] = forces[c] + cols[d][g] * at[index[c][d]]
        for c in range(3):
            force_out[c, :, lanes] = forces[c]
    fetch(((stress_out, stress_hbm), (force_out, force_hbm)), sems)


def swap(first, second, axis, count):
    even = [(i, i ^ 1) for i in range(count)]
    odd = [(i, i + 1 if i % 2 else i - 1) for i in range(1, count - 1)]
    if axis == "gx":
        turns = lax.axis_size("gy")
        even, odd = (
            [(a * turns + t, b * turns + t) for t in range(turns) for a, b in (one, two)[t % 2]]
            for one, two in ((even, odd), (odd, even))
        )
        axis = ("gx", "gy")
    a = lax.ppermute(first, axis, even)
    b = lax.ppermute(second, axis, odd)
    return a, b


def program(temps, cond, absorb, layers, owner, cell, de, st, lim):
    vm = lambda n: pltpu.VMEM((n, 128), F32)
    sx, sy, sz = (lax.axis_size(a) for a in ("gx", "gy", "gz"))
    cols, zpay, live = call(
        prep_kernel,
        (vm(512), vm(32), vm(8)),
        (temps.reshape(27, 16, 128), cond.reshape(16, 128), absorb.reshape(16, 128), layers),
        scratch=[
            pltpu.VMEM((27, 16, 128), F32), vm(16), vm(16), pltpu.SemaphoreType.DMA((3,)),
        ],
        far=(0, 1, 2, 3),
    )
    za, zb = swap(zpay, zpay, "gz", sz)
    xf, xs, hown = call(xpay_kernel, (vm(XROWS), vm(XROWS), vm(32)), (cols, za, zb))
    xa, xb = swap(xf, xs, "gx", sx)
    yf, ys = call(ypay_kernel, (vm(YROWS), vm(YROWS)), (cols, xa, xb, hown))
    ya, yb = swap(yf, ys, "gy", sy)
    m0, h0, yz, yzh, xtab, xhtab, old, bmat, own = call(
        pre_kernel,
        (
            vm(6144), vm(512), vm(144), vm(144), vm(192), vm(96), vm(128),
            pltpu.VMEM((256, 2048), jnp.bfloat16), pltpu.VMEM((16, 128), jnp.int32),
        ),
        (cols, hown, xa, xb, owner.reshape(16, 128), cell.reshape(16, 128)),
        scratch=[pltpu.VMEM((16, 128), jnp.int32), pltpu.SemaphoreType.DMA((2,))],
        far=(4, 5),
    )
    t_new, pay, _, _ = call(
        main_kernel,
        (pltpu.HBM((27, 16, 128), F32), vm(OWNERS * 18), vm(6144), vm(512)),
        (m0, h0, yz, yzh, xtab, xhtab, old, bmat, xa, xb, ya, yb, hown, own, live),
        scratch=[
            pltpu.VMEM((27, 16, 128), F32), pltpu.SemaphoreType.DMA((2,)), vm(6144), vm(512), vm(192), vm(192), vm(192), vm(192), vm(48), vm(144), vm(72), vm(128),
            pltpu.VMEM((272, 2048), jnp.bfloat16), vm(256),
        ],
        aliases={0: 2, 1: 3},
    )
    group = [(o + FIRST) % OWNERS for o in range(OWNERS)]
    got = lax.all_to_all(pay.reshape(OWNERS, 1, 2304), "gx", 0, 0, axis_index_groups=[group], tiled=True)
    stress, forces = call(
        mechanics_kernel,
        (pltpu.HBM((6, 8, 256), F32), pltpu.HBM((3, 8, 256), F32)),
        (got.reshape(OWNERS * 18, 128), de, st, lim.reshape(1, 256)),
        scratch=[pltpu.VMEM((6, 8, 256), F32), pltpu.VMEM((3, 8, 256), F32), pltpu.SemaphoreType.DMA((2,))],
    )
    return t_new.reshape(3, 3, 3, 4, 4, 128), stress, forces


def solution(mesh):
    cells = P(None, None, ("gx", "gy", "gz"))
    temps = P(None, None, None, "gx", "gy", "gz")
    block = P("gx", "gy", "gz")
    return jax.shard_map(
        program,
        mesh=mesh,
        in_specs=(
            temps, block, block, block, P("gx", "gy", "gz", None, None), P("gx", "gy", "gz", None),
            cells, cells, P(("gx", "gy", "gz")),
        ),
        out_specs=(temps, cells, cells),
        check_vma=False,
    )
```

```python
import functools
import math

import jax
import jax.numpy as jnp
import numpy as np
from jax import lax
from jax.experimental import pallas as pl
from jax.experimental.pallas import tpu as pltpu
from jax.sharding import PartitionSpec as P


STEPS = 4
DT = 0.003
PENALTY = 3.0
HEAT = 100.0 * (2.0 / 3.0)
EXPANSION = 0.02
MU = 100.0 / 2.6
LAME = 30.0 / 0.52
HARD = 10.0
NX, NY, NZ = 64, 32, 512
PX, PY, PZ = 4, 4, 128
OWNERS, CELLS = 16, 256
FIRST = 8
F32 = jnp.float32

LAM = (0.0, 12.0, 24.0)
ROWS = 29
FAR = 20

X1 = [ROWS * y for y in range(4)]
X2 = [4 * ROWS + FAR * y for y in range(4)]
XH = 4 * ROWS + 4 * FAR
XROWS = 232
Y1, Y2 = X1, X2
NEAR = [(0, XH), (1, XH + ROWS)]
EDGE = [(side, xd, 3 - xd, XH + 2 * ROWS + 4 * (2 * side + xd - 1)) for side in (0, 1) for xd in (1, 2)]
YH = [XH + 2 * ROWS + 16, XH + 3 * ROWS + 16]
YROWS = 328


def mode(i, j, l):
    return 9 * i + 3 * j + l


def call(kernel, outs, args, scratch=(), far=(), aliases=None):
    def place(n, a):
        return a if a.size == 1 else pltpu.with_memory_space_constraint(a, pltpu.HBM if n in far else pltpu.VMEM)

    return pl.pallas_call(
        kernel,
        out_shape=outs,
        in_specs=[
            pl.BlockSpec(memory_space=pltpu.SMEM if a.size == 1 else pltpu.HBM if n in far else pltpu.VMEM)
            for n, a in enumerate(args)
        ],
        out_specs=tuple(pl.BlockSpec(memory_space=o.memory_space) for o in outs),
        input_output_aliases=aliases or {},
        compiler_params=pltpu.CompilerParams(vmem_limit_bytes=24 << 20),
        scratch_shapes=list(scratch),
    )(*[place(n, a) for n, a in enumerate(args)])


def fetch(pairs, sems):
    copies = [pltpu.make_async_copy(a, b, sems.at[n]) for n, (a, b) in enumerate(pairs)]
    for c in copies:
        c.start()
    for c in copies:
        c.wait()


def lane_iota(rows):
    return lax.broadcasted_iota(jnp.int32, (rows, 128), 1)


def row_iota(rows):
    return lax.broadcasted_iota(jnp.int32, (rows, 128), 0)


def modal(a, b, c):
    s = a + c
    return (s + 4.0 * b) * (1.0 / 6.0), (c - a) * 0.5, (s - 2.0 * b) * (1.0 / 3.0)


def modal_grid(values):
    for stride in (9, 3, 1):
        out = [None] * 27
        for base in range(27):
            if base // stride % 3 == 0:
                ids = [base + stride * t for t in range(3)]
                for q, r in zip(ids, modal(*[values[q] for q in ids])):
                    out[q] = r
        values = out
    return values


def nodal_grid(values):
    for stride in (9, 3, 1):
        out = [None] * 27
        for base in range(27):
            if base // stride % 3 == 0:
                al, be, ga = (values[base + stride * t] for t in range(3))
                e = al + ga
                out[base], out[base + stride], out[base + 2 * stride] = e - be, al - 0.5 * ga, e + be
        values = out
    return values


def prep_kernel(t_in, k_in, a_in, lay_ref, cols_ref, zpay_ref, live_ref, t_ref, k_ref, a_ref, sems):
    fetch(((t_in, t_ref), (k_in, k_ref), (a_in, a_ref)), sems)
    m = (lane_iota(8) < lay_ref[0, 0, 0]).astype(F32)
    live_ref[...] = m
    lane = lane_iota(32)
    for h in range(2):
        rows = slice(8 * h, 8 * h + 8)
        modes = modal_grid([t_ref[n, rows, :] for n in range(27)])
        modes.append(k_ref[rows, :] * m)
        modes.append(a_ref[rows, :] * m * (DT * HEAT))
        for n, v in enumerate(modes):
            cols_ref[pl.ds(8 * h * 32 + n, 8, stride=32), :] = v
    zero = jnp.zeros((3, 128), F32)
    acc = jnp.zeros((32, 128), F32)
    for c in range(16):
        cols_ref[c * 32 + 29 : c * 32 + 32, :] = zero
    for c in range(16):
        x, y = c // 4, c % 4
        start = y * 32 + x * 8
        v = pltpu.roll(cols_ref[c * 32 : c * 32 + 32, :], (4 + start) % 128, axis=1)
        acc = jnp.where((lane >= start) & (lane < start + 8), v, acc)
    zpay_ref[...] = acc


def upper_first(axis):
    at = lax.axis_index(axis)
    return (at + lax.axis_index("gy") if axis == "gx" else at) % 2 == 0


def by_parity(axis, write, first, second):
    even = upper_first(axis)

    @pl.when(even)
    def _():
        write(first, second)

    @pl.when(jnp.logical_not(even))
    def _():
        write(second, first)


def put(dst, at, parts):
    for part in parts:
        dst[at : at + part.shape[0], :] = part
        at += part.shape[0]


def far_modes(column, axis, sign):
    half = 0.5 * sign
    if axis == 0:
        odd = half * column[9:18]
        return [column[0:9] + odd, column[18:27] + odd, column[27:29]]
    out = []
    for i in range(3):
        odd = half * column[9 * i + 3 : 9 * i + 6]
        out += [column[9 * i : 9 * i + 3] + odd, column[9 * i + 6 : 9 * i + 9] + odd]
    return out + [column[27:29]]


def xhalo_block(even, xa_ref, xb_ref, side, at, rows):
    a, b = xa_ref[at : at + rows, :], xb_ref[at : at + rows, :]
    return jnp.where(even, b, a) if side == 0 else jnp.where(even, a, b)


def xpay_kernel(cols_ref, za_ref, zb_ref, first_ref, second_ref, h_ref):
    even = upper_first("gz")
    idx = lane_iota(32) % 8
    za, zb = za_ref[...], zb_ref[...]
    upper = jnp.where(even, za, zb)
    lower = jnp.where(even, zb, za)
    own = jnp.where(idx < 4, lower, upper)
    h_ref[...] = own

    def write(upper_ref, lower_ref):
        for y in range(4):
            column = [cols_ref[(x * 4 + y) * 32 : (x * 4 + y) * 32 + ROWS, :] for x in range(4)]
            put(upper_ref, X1[y], [column[3]])
            put(lower_ref, X1[y], [column[0]])
            put(upper_ref, X2[y], far_modes(column[2], 0, 1.0))
            put(lower_ref, X2[y], far_modes(column[1], 0, -1.0))
        for ref in (upper_ref, lower_ref):
            ref[XH : XH + ROWS, :] = own[0:ROWS]

    by_parity("gx", write, first_ref, second_ref)


def ypay_kernel(cols_ref, xa_ref, xb_ref, h_ref, first_ref, second_ref):
    halo = functools.partial(xhalo_block, upper_first("gx"), xa_ref, xb_ref)

    def edge(side, xd, y, ysign):
        if xd == 1:
            c = [halo(side, X1[y] + 9 * i, 9) for i in range(3)]
            face, k = c[0] + c[2] + (1.0 if side == 0 else -1.0) * c[1], halo(side, X1[y] + 27, 1)
        else:
            face, k = halo(side, X2[y], 9) + halo(side, X2[y] + 9, 9), halo(side, X2[y] + 18, 1)
        return [face[0:3] + face[6:9] + ysign * face[3:6], k]

    def write(upper_ref, lower_ref):
        for x in range(4):
            column = [cols_ref[(x * 4 + y) * 32 : (x * 4 + y) * 32 + ROWS, :] for y in range(4)]
            put(upper_ref, Y1[x], [column[3]])
            put(lower_ref, Y1[x], [column[0]])
            put(upper_ref, Y2[x], far_modes(column[2], 1, 1.0))
            put(lower_ref, Y2[x], far_modes(column[1], 1, -1.0))
        for side, at in NEAR:
            put(upper_ref, at, [halo(side, X1[3], ROWS)])
            put(lower_ref, at, [halo(side, X1[0], ROWS)])
        for side, xd, d, at in EDGE:
            put(upper_ref, at, edge(side, xd, 4 - d, 1.0))
            put(lower_ref, at, edge(side, xd, d - 1, -1.0))
        beside = jnp.where(lane_iota(ROWS) // 8 % 4 < 2, halo(1, XH, ROWS), halo(0, XH, ROWS))
        for ref in (upper_ref, lower_ref):
            ref[YH[0] : YH[0] + ROWS, :] = h_ref[0:ROWS, :]
            ref[YH[1] : YH[1] + ROWS, :] = beside

    by_parity("gy", write, first_ref, second_ref)


def couple(k1, k2):
    return (2.0 * PENALTY * DT) * k1 * k2 / jnp.maximum(k1 + k2, 1.0)


def roll_lanes(v, shift):
    return pltpu.roll(v, shift, axis=1)


def wide(v, n):
    return v if n == 8 else jnp.concatenate([v, v], axis=0)


def shift_rows(v, up):
    return pltpu.roll(v, 7 if up else 1, axis=0)


def line_faces(values, stride):
    out = []
    for base in range(27):
        if base // stride % 3 == 0:
            e = values[base] + values[base + 2 * stride]
            out.append((e - values[base + stride], e + values[base + stride]))
    return out


def slot(y):
    return (y + 2) % 16


def advance(values, kappa, heats, yz, fluxes):
    factor = {}
    for total in sorted({LAM[i] + LAM[j] + LAM[l] for i in range(3) for j in range(3) for l in range(3)}):
        factor[total] = 1.0 - kappa * total if total else None
    terms = []
    for lines in fluxes:
        per = []
        for low, high in lines:
            gain, both = low - high, low + high
            per.append((gain, -3.0 * both, 2.0 * gain))
        terms.append(per)
    out = []
    for i in range(3):
        for j in range(3):
            for l in range(3):
                v = values[mode(i, j, l)]
                f = factor[LAM[i] + LAM[j] + LAM[l]]
                v = v if f is None else v * f
                v = v + heats[i] * yz[3 * j + l]
                v = v + (terms[0][3 * j + l][i] + terms[1][3 * i + l][j]) + terms[2][3 * i + j][l]
                out.append(v)
    return out


def gauss_exp(offset, near, far):
    scaled = offset * jnp.where(offset >= 0.0, 1.0 / near, 1.0 / far)
    return jnp.exp(-3.0 * (scaled * scaled))


def place(m0, x, y, block):
    m0[pl.ds((x + 4) * 512 + slot(y), ROWS, stride=16), :] = block


def place_h(h0, row, y, blocks):
    lane = lane_iota(ROWS)
    rolled = [roll_lanes(b, (32 * n - 32 * y) % 128) if (n - y) % 4 else b for n, b in enumerate(blocks)]
    v = jnp.where(lane < 32, rolled[0], jnp.where(lane < 64, rolled[1], rolled[2]))
    h0[pl.ds(row, ROWS, stride=16), :] = jnp.where(lane < 96, v, 0.0)


def pair(ref, p, m):
    a = ref[pl.ds((4 + 2 * p) * 512 + 16 * m, 8), :]
    b = ref[pl.ds((5 + 2 * p) * 512 + 16 * m, 8), :]
    return jnp.where(row_iota(8) < 4, pltpu.roll(a, 6, axis=0), pltpu.roll(b, 2, axis=0))


LOW = [mode(i, j, l) for i in range(2) for j in range(2) for l in range(2)]


def line_modes(base, centre, near, far):
    return modal(*[gauss_exp(base + 0.5 * n - centre, near, far) for n in range(3)])


def pre_kernel(
    cols_ref, h_ref, xa_ref, xb_ref, own_in, cell_in,
    m0, h0, yz, yzh, xtab, xhtab, old, bmat, own_out,
    cell_ref, sems,
):
    gx, gy, gz = lax.axis_index("gx"), lax.axis_index("gy"), lax.axis_index("gz")
    even_x = upper_first("gx")
    fetch(((own_in, own_out), (cell_in, cell_ref)), sems)

    def clear(xi, _):
        for m in range(ROWS):
            m0[pl.ds(pl.multiple_of(xi * 512 + 16 * m, 16), 8), :] = jnp.zeros((8, 128), F32)
        return 0

    lax.fori_loop(1, 11, clear, 0)
    h0[...] = jnp.zeros((512, 128), F32)
    xhalo = functools.partial(xhalo_block, even_x, xa_ref, xb_ref)
    for c in range(16):
        place(m0, c // 4, c % 4, cols_ref[c * 32 : c * 32 + ROWS, :])
    for side in (0, 1):
        for y in range(4):
            place(m0, -1 if side == 0 else 4, y, xhalo(side, X1[y], ROWS))
            block = xhalo(side, X2[y], FAR)
            at = (2 if side == 0 else 9) * 512 + slot(y)
            m0[pl.ds(at, 9, stride=16), :] = block[0:9]
            m0[pl.ds(at + 18 * 16, 11, stride=16), :] = block[9:20]
    blocks = [xhalo(0, XH, ROWS), h_ref[0:ROWS, :], xhalo(1, XH, ROWS)]
    for y in range(4):
        place_h(h0, slot(y), y, blocks)

    lane16 = lane_iota(16)
    idx16 = lane16 % 8
    s16 = row_iota(16)
    ypos = (gy * PY + jnp.where(s16 < 12, s16 - 2, s16 - 18)).astype(F32)
    ymodes = line_modes(ypos, NY * 0.5, NY / 4.0, NY / 4.0)
    zpos = (gz * PZ + lane16).astype(F32)
    zmodes = line_modes(zpos, NZ * 0.75, NZ / 8.0, NZ / 8.0)
    zhpos = (gz * PZ + jnp.where(idx16 < 4, idx16 - 4, idx16 + 124)).astype(F32)
    zhmodes = line_modes(zhpos, NZ * 0.75, NZ / 8.0, NZ / 8.0)
    for j in range(3):
        for l in range(3):
            at = (3 * j + l) * 16
            yz[at : at + 16, :] = ymodes[j] * zmodes[l]
            yzh[at : at + 16, :] = ymodes[j] * zhmodes[l]
    for step in range(STEPS):
        centre = NX * 0.5 + step * NX / 16.0
        for t, v in enumerate(line_modes((gx * PX + s16 - 4).astype(F32), centre, NX / 8.0, NX / 4.0)):
            xtab[(3 * step + t) * 16 : (3 * step + t) * 16 + 16, :] = v
        for t, v in enumerate(line_modes((gx * PX + lane_iota(8) // 8 - 4).astype(F32), centre, NX / 8.0, NX / 4.0)):
            xhtab[(3 * step + t) * 8 : (3 * step + t) * 8 + 8, :] = v

    for g, m in enumerate(LOW):
        for p in range(2):
            old[16 * g + 8 * p : 16 * g + 8 * p + 8, :] = pair(m0, p, m)
    for c in range(16):
        cell = jnp.broadcast_to(cell_ref[c : c + 1, :], (CELLS, 128))
        hit = cell == row_iota(CELLS)
        bmat[:, 128 * c : 128 * c + 128] = jnp.where(hit, 1.0, 0.0).astype(jnp.bfloat16)


def main_kernel(
    m0_in, h0_in, yz, yzh, xtab, xhtab, old, bmat, xa_ref, xb_ref, ya_ref, yb_ref, h_ref, own_ref, live_ref,
    t_hbm, pay_out, m0, h0,
    t_out, sem, m1, h1, cx, cy, czu, czd, ch, gs, q_ref, inc, amat, csum,
):
    del m0_in, h0_in
    even_y = upper_first("gy")
    lane8 = lane_iota(8)
    zeros8 = jnp.zeros((8, 128), F32)

    def yhalo(side, at, rows):
        a, b = ya_ref[at : at + rows, :], yb_ref[at : at + rows, :]
        return jnp.where(even_y, b, a) if side == 0 else jnp.where(even_y, a, b)

    for side in (0, 1):
        out = [-d if side == 0 else 3 + d for d in range(3)]
        for x in range(4):
            place(m0, x, out[1], yhalo(side, Y1[x], ROWS))
            block = yhalo(side, Y2[x], FAR)
            at = (x + 4) * 512 + slot(out[2])
            for i in range(3):
                for j in (0, 1):
                    row = 6 * i + 3 * j
                    m0[pl.ds(at + (9 * i + 6 * j) * 16, 3, stride=16), :] = block[row : row + 3]
            m0[pl.ds(at + 27 * 16, 2, stride=16), :] = block[18:20]
        for xside, at in NEAR:
            place(m0, -1 if xside == 0 else 4, out[1], yhalo(side, at, ROWS))
        for xside, xd, d, at in EDGE:
            block = yhalo(side, at, 4)
            to = ((-xd if xside == 0 else 3 + xd) + 4) * 512 + slot(out[d])
            m0[pl.ds(to, 3, stride=16), :] = block[0:3]
            m0[pl.ds(to + 27 * 16, 1), :] = block[3:4]
        beside = yhalo(side, YH[1], ROWS)
        blocks = [beside, yhalo(side, YH[0], ROWS), beside]
        for d in (1, 2):
            place_h(h0, slot(out[d]), out[d] % 4, blocks)

    idx8 = lane8 % 8
    kh = h0[27 * 16 : 27 * 16 + 8, :]
    last_row = row_iota(8) == 7
    gk_src = jnp.where(idx8 == 5, roll_lanes(kh, 2), kh)
    ch[0:8, :] = couple(kh, roll_lanes(kh, 120))
    ch[16:24, :] = jnp.where(last_row, 0.0, couple(kh, shift_rows(kh, True)))
    ch[32:40, :] = jnp.where((idx8 == 3) | (idx8 == 7), 0.0, couple(kh, roll_lanes(kh, 127)))
    ks = [m0[xi * 512 + 27 * 16 : xi * 512 + 27 * 16 + 8, :] for xi in range(1, 11)]
    for xi in range(1, 10):
        k, at = ks[xi - 1], slice(xi * 16, xi * 16 + 8)
        cx[at, :] = couple(k, ks[xi])
        if xi == 1:
            continue
        gk = roll_lanes(gk_src, 123 - xi * 8)
        cy[at, :] = jnp.where(last_row, 0.0, couple(k, shift_rows(k, True)))
        czu[at, :] = couple(k, jnp.where(lane8 == 127, gk, roll_lanes(k, 127)))
        czd[at, :] = couple(k, gk)

    def rows_of(ref, xi, n):
        return [ref[pl.ds(pl.multiple_of(xi * 512 + 16 * m, 8), n), :] for m in range(27)]

    def at_x(ref, xi, n):
        return ref[pl.ds(pl.multiple_of(xi * 16, 8), n), :]

    def table(ref, n):
        return [ref[16 * t : 16 * t + n, :] for t in range(9)]

    groups = [
        [(2, 10)],
        [(3, 9)],
        [(3, 9)],
        [(4, 6), (6, 8)],
    ]
    live = live_ref[...]
    out_copies = [
        pltpu.make_async_copy(t_out.at[:, 8 * p : 8 * p + 8, :], t_hbm.at[:, 8 * p : 8 * p + 8, :], sem.at[p])
        for p in range(2)
    ]

    def finish(ref, p):
        modes = [pair(ref, p, m) for m in range(27)]
        for n, v in enumerate(nodal_grid(modes)):
            t_out[n, 8 * p : 8 * p + 8, :] = v
        out_copies[p].start()
        for g, m in enumerate(LOW):
            at = 16 * g + 8 * p
            inc[at : at + 8, :] = (modes[m] - old[at : at + 8, :]) * live

    src, dst, hsrc, hdst = m0, m1, h0, h1
    for step in range(STEPS):
        last = step == STEPS - 1
        hn = 8
        hv = [hsrc[16 * m : 16 * m + hn, :] for m in range(27)]
        lane_h = lane_iota(hn)
        idx_h = lane_h % 8
        hz = line_faces(hv, 1)
        for t, (low, high) in enumerate(hz):
            gs[16 * t : 16 * t + hn, :] = jnp.where(idx_h == 5, roll_lanes(high, 2), low)
        if not last:
            for t in range(9):
                q_ref[8 * t : 8 * t + 8, :] = zeros8

        n = 8
        for first, end in groups[step]:
            lane_n = lane_iota(n)

            def xflux(here, there, xi, n=n):
                c = at_x(cx, xi, n)
                return tuple(c * (a[1] - b[0]) for a, b in zip(line_faces(here, 9), line_faces(there, 9)))

            def body(xi, carry, n=n, src=src, dst=dst, step=step, last=last, lane_n=lane_n):
                left = carry
                values = rows_of(src, xi, n)
                following = rows_of(src, xi + 1, n)
                right = xflux(values, following, xi, n)
                kappa = DT * src_k(xi, n)
                heat = src_a(xi, n)
                xm = [xtab[pl.ds((3 * step + t) * 16 + xi, 1), :] for t in range(3)]
                heats = [heat * jnp.broadcast_to(v, (n, 128)) for v in xm]
                c = at_x(cy, xi, n)
                yf = []
                for low, high in line_faces(values, 3):
                    up = c * (high - shift_rows(low, True))
                    yf.append((shift_rows(up, False), up))
                cu, cd = at_x(czu, xi, n), at_x(czd, xi, n)
                zf = []
                shift = 123 - xi * 8
                mine = (lane8 == xi * 8 + 4) | (lane8 == xi * 8 + 5)
                for t, (low, high) in enumerate(line_faces(values, 1)):
                    g = roll_lanes(gs[16 * t : 16 * t + n, :], shift)
                    up = cu * (high - jnp.where(lane_n == 127, g, roll_lanes(low, 127)))
                    down = jnp.where(lane_n == 0, cd * (g - low), roll_lanes(up, 1))
                    zf.append((down, up))
                    if not last:
                        back = roll_lanes(jnp.where(lane8 == 127, up[0:8], down[0:8]), xi * 8 + 5)
                        q_ref[8 * t : 8 * t + 8, :] = jnp.where(mine, back, q_ref[8 * t : 8 * t + 8, :])
                out = advance(values, kappa, heats, table(yz, n), (list(zip(left, right)), yf, zf))
                for m, v in enumerate(out):
                    dst[pl.ds(pl.multiple_of(xi * 512 + 16 * m, 8), n), :] = v
                return right

            def src_k(xi, n):
                return m0[pl.ds(pl.multiple_of(xi * 512 + 27 * 16, 8), n), :]

            def src_a(xi, n):
                return m0[pl.ds(pl.multiple_of(xi * 512 + 28 * 16, 8), n), :]

            left = xflux(rows_of(src, first - 1, n), rows_of(src, first, n), first - 1, n)
            if end - first <= 2:
                for xi in range(first, end):
                    left = body(xi, left)
                if last:
                    finish(dst, first // 2 - 2)
            else:
                lax.fori_loop(0, (end - first) // 2, lambda t, c: body(first + 2 * t + 1, body(first + 2 * t, c)), left)

        if not last:
            n = 8
            inner = [v[0:8] for v in hv]
            idx_n = lane_iota(n) % 8
            xm = [xhtab[(3 * step + t) * 8 : (3 * step + t) * 8 + 8, :] for t in range(3)]
            heat = h0[28 * 16 : 28 * 16 + n, :]
            heats = [heat * wide(v, n) for v in xm]
            c = ch[0:n, :]
            xf = []
            for low, high in line_faces(inner, 9):
                up = c * (high - roll_lanes(low, 120))
                xf.append((roll_lanes(up, 8), up))
            c = ch[16 : 16 + n, :]
            yf = []
            for low, high in line_faces(inner, 3):
                up = c * (high - shift_rows(low, True))
                yf.append((shift_rows(up, False), up))
            c = ch[32 : 32 + n, :]
            zf = []
            for t, (low, high) in enumerate(line_faces(inner, 1)):
                up = c * (high - roll_lanes(low, 127))
                q = wide(q_ref[8 * t : 8 * t + 8, :], n)
                down = jnp.where(idx_n == 4, q, roll_lanes(up, 1))
                zf.append((down, jnp.where(idx_n == 3, roll_lanes(q, 126), up)))
            kappa = DT * h0[27 * 16 : 27 * 16 + n, :]
            out = advance(inner, kappa, heats, table(yzh, n), (xf, yf, zf))
            for m, v in enumerate(out):
                hdst[16 * m : 16 * m + n, :] = v
        src, dst, hsrc, hdst = dst, src, hdst, hsrc

    slots = (row_iota(16) + FIRST) % OWNERS
    for c in range(16):
        lanes = slice(128 * c, 128 * c + 128)
        v = inc[pl.ds(c, 8, stride=16), :]
        hi = v.astype(jnp.bfloat16).astype(F32)
        lo = v - hi
        owner = jnp.broadcast_to(own_ref[c : c + 1, :], (8, 128))
        picks = [owner == (o + FIRST) % OWNERS for o in range(OWNERS)]
        amat[0:128, lanes] = jnp.concatenate([jnp.where(k, hi, 0.0) for k in picks], axis=0).astype(jnp.bfloat16)
        amat[128:256, lanes] = jnp.concatenate([jnp.where(k, lo, 0.0) for k in picks], axis=0).astype(jnp.bfloat16)
        owner16 = jnp.broadcast_to(own_ref[c : c + 1, :], (16, 128))
        amat[256:272, lanes] = jnp.where(owner16 == slots, wide(live, 16), 0.0).astype(jnp.bfloat16)
    total = lax.dot_general(
        amat[...], bmat[...], (((1,), (1,)), ((), ())), preferred_element_type=F32
    )
    csum[0:128, :] = (total[0:128] + total[128:256])[:, 0:128]
    csum[128:256, :] = (total[0:128] + total[128:256])[:, 128:256]
    for h in range(2):
        for g in range(8):
            pay_out[pl.ds(2 * g + h, 16, stride=18), :] = csum[pl.ds(128 * h + g, 16, stride=8), :]
        pay_out[pl.ds(16 + h, 16, stride=18), :] = total[256:272, 128 * h : 128 * h + 128]
    for c in out_copies:
        c.wait()


def gradient_table():
    spots = [0.5 - 0.5 / math.sqrt(3.0), 0.5 + 0.5 / math.sqrt(3.0)]
    out = np.zeros((3, 8, 8), np.float32)
    for node in range(8):
        corner = [node // 4, node // 2 % 2, node % 2]
        for point in range(8):
            place = [spots[point // 4], spots[point // 2 % 2], spots[point % 2]]
            values = [place[k] if corner[k] else 1.0 - place[k] for k in range(3)]
            slopes = [1.0 if corner[k] else -1.0 for k in range(3)]
            out[0, node, point] = slopes[0] * values[1] * values[2] / 8.0
            out[1, node, point] = values[0] * slopes[1] * values[2] / 8.0
            out[2, node, point] = values[0] * values[1] * slopes[2] / 8.0
    return out


def column(values):
    rows = row_iota(8)
    out = jnp.full((8, 128), float(values[7]), F32)
    for r in range(7):
        out = jnp.where(rows == r, float(values[r]), out)
    return out


def mechanics_kernel(got_ref, de_ref, st_ref, lim_ref, stress_hbm, force_hbm, stress_out, force_out, sems):
    sums = got_ref[0:18, :]
    for s in range(1, OWNERS):
        sums = sums + got_ref[18 * s : 18 * s + 18, :]
    root = 1.0 / math.sqrt(3.0)
    rows = row_iota(8)
    signs = [jnp.where(rows // w % 2 == 0, -root, root) for w in (4, 2, 1)]
    table = gradient_table()
    cols = [[column(table[d, :, g]) for g in range(8)] for d in range(3)]
    for h in range(2):
        lanes = slice(128 * h, 128 * h + 128)
        inv = 1.0 / jnp.maximum(sums[16 + h : 17 + h], 1.0)

        def row(m):
            return jnp.broadcast_to(sums[2 * m + h : 2 * m + h + 1] * inv, (8, 128))

        z = [row(2 * n) + signs[2] * row(2 * n + 1) for n in range(4)]
        y = [z[2 * n] + signs[1] * z[2 * n + 1] for n in range(2)]
        strain = EXPANSION * (y[0] + signs[0] * y[1])
        normal = [de_ref[k, :, lanes] - strain for k in range(3)]
        volume = normal[0] + normal[1] + normal[2]
        trial = [st_ref[k, :, lanes] + LAME * volume + 2.0 * MU * normal[k] for k in range(3)]
        shear = [st_ref[k, :, lanes] + 2.0 * MU * de_ref[k, :, lanes] for k in range(3, 6)]
        pressure = (trial[0] + trial[1] + trial[2]) * (1.0 / 3.0)
        dev = [t - pressure for t in trial]
        squares = dev[0] * dev[0] + dev[1] * dev[1] + dev[2] * dev[2]
        squares = squares + 2.0 * (shear[0] * shear[0] + shear[1] * shear[1] + shear[2] * shear[2])
        equivalent = jnp.sqrt(1.5 * squares)
        limit = jnp.broadcast_to(lim_ref[0:1, lanes], (8, 128))
        plastic = jnp.maximum(equivalent - limit, 0.0) * (1.0 / (3.0 * MU + HARD))
        factor = 1.0 - (3.0 * MU) * plastic / jnp.maximum(equivalent, limit)
        stress = [pressure + factor * d for d in dev] + [factor * s for s in shear]
        for k in range(6):
            stress_out[k, :, lanes] = stress[k]
        index = [[0, 5, 4], [5, 1, 3], [4, 3, 2]]
        forces = [jnp.zeros((8, 128), F32)] * 3
        for g in range(8):
            at = [jnp.broadcast_to(s[g : g + 1], (8, 128)) for s in stress]
            for c in range(3):
                for d in range(3):
                    forces[c] = forces[c] + cols[d][g] * at[index[c][d]]
        for c in range(3):
            force_out[c, :, lanes] = forces[c]
    fetch(((stress_out, stress_hbm), (force_out, force_hbm)), sems)


def swap(first, second, axis, count):
    even = [(i, i ^ 1) for i in range(count)]
    odd = [(i, i + 1 if i % 2 else i - 1) for i in range(1, count - 1)]
    if axis == "gx":
        turns = lax.axis_size("gy")
        even, odd = (
            [(a * turns + t, b * turns + t) for t in range(turns) for a, b in (one, two)[t % 2]]
            for one, two in ((even, odd), (odd, even))
        )
        axis = ("gx", "gy")
    a = lax.ppermute(first, axis, even)
    b = lax.ppermute(second, axis, odd)
    return a, b


def program(temps, cond, absorb, layers, owner, cell, de, st, lim):
    vm = lambda n: pltpu.VMEM((n, 128), F32)
    sx, sy, sz = (lax.axis_size(a) for a in ("gx", "gy", "gz"))
    cols, zpay, live = call(
        prep_kernel,
        (vm(512), vm(32), vm(8)),
        (temps.reshape(27, 16, 128), cond.reshape(16, 128), absorb.reshape(16, 128), layers),
        scratch=[
            pltpu.VMEM((27, 16, 128), F32), vm(16), vm(16), pltpu.SemaphoreType.DMA((3,)),
        ],
        far=(0, 1, 2, 3),
    )
    za, zb = swap(zpay, zpay, "gz", sz)
    xf, xs, hown = call(xpay_kernel, (vm(XROWS), vm(XROWS), vm(32)), (cols, za, zb))
    xa, xb = swap(xf, xs, "gx", sx)
    yf, ys = call(ypay_kernel, (vm(YROWS), vm(YROWS)), (cols, xa, xb, hown))
    ya, yb = swap(yf, ys, "gy", sy)
    m0, h0, yz, yzh, xtab, xhtab, old, bmat, own = call(
        pre_kernel,
        (
            vm(6144), vm(512), vm(144), vm(144), vm(192), vm(96), vm(128),
            pltpu.VMEM((256, 2048), jnp.bfloat16), pltpu.VMEM((16, 128), jnp.int32),
        ),
        (cols, hown, xa, xb, owner.reshape(16, 128), cell.reshape(16, 128)),
        scratch=[pltpu.VMEM((16, 128), jnp.int32), pltpu.SemaphoreType.DMA((2,))],
        far=(4, 5),
    )
    t_new, pay, _, _ = call(
        main_kernel,
        (pltpu.HBM((27, 16, 128), F32), vm(OWNERS * 18), vm(6144), vm(512)),
        (m0, h0, yz, yzh, xtab, xhtab, old, bmat, xa, xb, ya, yb, hown, own, live),
        scratch=[
            pltpu.VMEM((27, 16, 128), F32), pltpu.SemaphoreType.DMA((2,)), vm(6144), vm(512), vm(192), vm(192), vm(192), vm(192), vm(48), vm(144), vm(72), vm(128),
            pltpu.VMEM((272, 2048), jnp.bfloat16), vm(256),
        ],
        aliases={0: 2, 1: 3},
    )
    group = [(o + FIRST) % OWNERS for o in range(OWNERS)]
    got = lax.all_to_all(pay.reshape(OWNERS, 1, 2304), "gx", 0, 0, axis_index_groups=[group], tiled=True)
    stress, forces = call(
        mechanics_kernel,
        (pltpu.HBM((6, 8, 256), F32), pltpu.HBM((3, 8, 256), F32)),
        (got.reshape(OWNERS * 18, 128), de, st, lim.reshape(1, 256)),
        scratch=[pltpu.VMEM((6, 8, 256), F32), pltpu.VMEM((3, 8, 256), F32), pltpu.SemaphoreType.DMA((2,))],
    )
    return t_new.reshape(3, 3, 3, 4, 4, 128), stress, forces


def solution(mesh):
    cells = P(None, None, ("gx", "gy", "gz"))
    temps = P(None, None, None, "gx", "gy", "gz")
    block = P("gx", "gy", "gz")
    return jax.shard_map(
        program,
        mesh=mesh,
        in_specs=(
            temps, block, block, block, P("gx", "gy", "gz", None, None), P("gx", "gy", "gz", None),
            cells, cells, P(("gx", "gy", "gz")),
        ),
        out_specs=(temps, cells, cells),
        check_vma=False,
    )
```

```python
import functools
import math

import jax
import jax.numpy as jnp
import numpy as np
from jax import lax
from jax.experimental import pallas as pl
from jax.experimental.pallas import tpu as pltpu
from jax.sharding import PartitionSpec as P


STEPS = 4
DT = 0.003
PENALTY = 3.0
HEAT = 100.0 * (2.0 / 3.0)
EXPANSION = 0.02
MU = 100.0 / 2.6
LAME = 30.0 / 0.52
HARD = 10.0
NX, NY, NZ = 64, 32, 512
PX, PY, PZ = 4, 4, 128
OWNERS, CELLS = 16, 256
FIRST = 8
F32 = jnp.float32

LAM = (0.0, 12.0, 24.0)
ROWS = 29
FAR = 20

X1 = [ROWS * y for y in range(4)]
X2 = [4 * ROWS + FAR * y for y in range(4)]
XH = 4 * ROWS + 4 * FAR
XROWS = 232
Y1, Y2 = X1, X2
NEAR = [(0, XH), (1, XH + ROWS)]
EDGE = [(side, xd, 3 - xd, XH + 2 * ROWS + 4 * (2 * side + xd - 1)) for side in (0, 1) for xd in (1, 2)]
YH = [XH + 2 * ROWS + 16, XH + 3 * ROWS + 16]
YROWS = 328


def mode(i, j, l):
    return 9 * i + 3 * j + l


def call(kernel, outs, args, scratch=(), far=(), aliases=None):
    def place(n, a):
        return a if a.size == 1 else pltpu.with_memory_space_constraint(a, pltpu.HBM if n in far else pltpu.VMEM)

    return pl.pallas_call(
        kernel,
        out_shape=outs,
        in_specs=[
            pl.BlockSpec(memory_space=pltpu.SMEM if a.size == 1 else pltpu.HBM if n in far else pltpu.VMEM)
            for n, a in enumerate(args)
        ],
        out_specs=tuple(pl.BlockSpec(memory_space=o.memory_space) for o in outs),
        input_output_aliases=aliases or {},
        compiler_params=pltpu.CompilerParams(vmem_limit_bytes=24 << 20),
        scratch_shapes=list(scratch),
    )(*[place(n, a) for n, a in enumerate(args)])


def fetch(pairs, sems):
    copies = [pltpu.make_async_copy(a, b, sems.at[n]) for n, (a, b) in enumerate(pairs)]
    for c in copies:
        c.start()
    for c in copies:
        c.wait()


def lane_iota(rows):
    return lax.broadcasted_iota(jnp.int32, (rows, 128), 1)


def row_iota(rows):
    return lax.broadcasted_iota(jnp.int32, (rows, 128), 0)


def modal(a, b, c):
    s = a + c
    return (s + 4.0 * b) * (1.0 / 6.0), (c - a) * 0.5, (s - 2.0 * b) * (1.0 / 3.0)


def modal_grid(values):
    for stride in (9, 3, 1):
        out = [None] * 27
        for base in range(27):
            if base // stride % 3 == 0:
                ids = [base + stride * t for t in range(3)]
                for q, r in zip(ids, modal(*[values[q] for q in ids])):
                    out[q] = r
        values = out
    return values


def nodal_grid(values):
    for stride in (9, 3, 1):
        out = [None] * 27
        for base in range(27):
            if base // stride % 3 == 0:
                al, be, ga = (values[base + stride * t] for t in range(3))
                e = al + ga
                out[base], out[base + stride], out[base + 2 * stride] = e - be, al - 0.5 * ga, e + be
        values = out
    return values


def prep_kernel(t_in, k_in, a_in, lay_ref, cols_ref, zpay_ref, live_ref, t_ref, k_ref, a_ref, sems):
    fetch(((t_in, t_ref), (k_in, k_ref), (a_in, a_ref)), sems)
    m = (lane_iota(8) < lay_ref[0, 0, 0]).astype(F32)
    live_ref[...] = m
    lane = lane_iota(32)
    for h in range(2):
        rows = slice(8 * h, 8 * h + 8)
        modes = modal_grid([t_ref[n, rows, :] for n in range(27)])
        modes.append(k_ref[rows, :] * m)
        modes.append(a_ref[rows, :] * m * (DT * HEAT))
        for n, v in enumerate(modes):
            cols_ref[pl.ds(8 * h * 32 + n, 8, stride=32), :] = v
    zero = jnp.zeros((3, 128), F32)
    acc = jnp.zeros((32, 128), F32)
    for c in range(16):
        cols_ref[c * 32 + 29 : c * 32 + 32, :] = zero
    for c in range(16):
        x, y = c // 4, c % 4
        start = y * 32 + x * 8
        v = pltpu.roll(cols_ref[c * 32 : c * 32 + 32, :], (4 + start) % 128, axis=1)
        acc = jnp.where((lane >= start) & (lane < start + 8), v, acc)
    zpay_ref[...] = acc


def upper_first(axis):
    at = lax.axis_index(axis)
    return (at + lax.axis_index("gy") if axis == "gx" else at) % 2 == 0


def by_parity(axis, write, first, second):
    even = upper_first(axis)

    @pl.when(even)
    def _():
        write(first, second)

    @pl.when(jnp.logical_not(even))
    def _():
        write(second, first)


def put(dst, at, parts):
    for part in parts:
        dst[at : at + part.shape[0], :] = part
        at += part.shape[0]


def far_modes(column, axis, sign):
    half = 0.5 * sign
    if axis == 0:
        odd = half * column[9:18]
        return [column[0:9] + odd, column[18:27] + odd, column[27:29]]
    out = []
    for i in range(3):
        odd = half * column[9 * i + 3 : 9 * i + 6]
        out += [column[9 * i : 9 * i + 3] + odd, column[9 * i + 6 : 9 * i + 9] + odd]
    return out + [column[27:29]]


def xhalo_block(even, xa_ref, xb_ref, side, at, rows):
    a, b = xa_ref[at : at + rows, :], xb_ref[at : at + rows, :]
    return jnp.where(even, b, a) if side == 0 else jnp.where(even, a, b)


def xpay_kernel(cols_ref, za_ref, zb_ref, first_ref, second_ref, h_ref):
    even = upper_first("gz")
    idx = lane_iota(32) % 8
    za, zb = za_ref[...], zb_ref[...]
    upper = jnp.where(even, za, zb)
    lower = jnp.where(even, zb, za)
    own = jnp.where(idx < 4, lower, upper)
    h_ref[...] = own

    def write(upper_ref, lower_ref):
        for y in range(4):
            column = [cols_ref[(x * 4 + y) * 32 : (x * 4 + y) * 32 + ROWS, :] for x in range(4)]
            put(upper_ref, X1[y], [column[3]])
            put(lower_ref, X1[y], [column[0]])
            put(upper_ref, X2[y], far_modes(column[2], 0, 1.0))
            put(lower_ref, X2[y], far_modes(column[1], 0, -1.0))
        for ref in (upper_ref, lower_ref):
            ref[XH : XH + ROWS, :] = own[0:ROWS]

    by_parity("gx", write, first_ref, second_ref)


def ypay_kernel(cols_ref, xa_ref, xb_ref, h_ref, first_ref, second_ref):
    halo = functools.partial(xhalo_block, upper_first("gx"), xa_ref, xb_ref)

    def edge(side, xd, y, ysign):
        if xd == 1:
            c = [halo(side, X1[y] + 9 * i, 9) for i in range(3)]
            face, k = c[0] + c[2] + (1.0 if side == 0 else -1.0) * c[1], halo(side, X1[y] + 27, 1)
        else:
            face, k = halo(side, X2[y], 9) + halo(side, X2[y] + 9, 9), halo(side, X2[y] + 18, 1)
        return [face[0:3] + face[6:9] + ysign * face[3:6], k]

    def write(upper_ref, lower_ref):
        for x in range(4):
            column = [cols_ref[(x * 4 + y) * 32 : (x * 4 + y) * 32 + ROWS, :] for y in range(4)]
            put(upper_ref, Y1[x], [column[3]])
            put(lower_ref, Y1[x], [column[0]])
            put(upper_ref, Y2[x], far_modes(column[2], 1, 1.0))
            put(lower_ref, Y2[x], far_modes(column[1], 1, -1.0))
        for side, at in NEAR:
            put(upper_ref, at, [halo(side, X1[3], ROWS)])
            put(lower_ref, at, [halo(side, X1[0], ROWS)])
        for side, xd, d, at in EDGE:
            put(upper_ref, at, edge(side, xd, 4 - d, 1.0))
            put(lower_ref, at, edge(side, xd, d - 1, -1.0))
        beside = jnp.where(lane_iota(ROWS) // 8 % 4 < 2, halo(1, XH, ROWS), halo(0, XH, ROWS))
        for ref in (upper_ref, lower_ref):
            ref[YH[0] : YH[0] + ROWS, :] = h_ref[0:ROWS, :]
            ref[YH[1] : YH[1] + ROWS, :] = beside

    by_parity("gy", write, first_ref, second_ref)


def couple(k1, k2):
    return (2.0 * PENALTY * DT) * k1 * k2 / jnp.maximum(k1 + k2, 1.0)


def roll_lanes(v, shift):
    return pltpu.roll(v, shift, axis=1)


def wide(v, n):
    return v if n == 8 else jnp.concatenate([v, v], axis=0)


def shift_rows(v, up):
    return pltpu.roll(v, 7 if up else 1, axis=0)


def line_faces(values, stride):
    out = []
    for base in range(27):
        if base // stride % 3 == 0:
            e = values[base] + values[base + 2 * stride]
            out.append((e - values[base + stride], e + values[base + stride]))
    return out


def slot(y):
    return (y + 2) % 16


def advance(values, kappa, heats, yz, fluxes):
    factor = {}
    for total in sorted({LAM[i] + LAM[j] + LAM[l] for i in range(3) for j in range(3) for l in range(3)}):
        factor[total] = 1.0 - kappa * total if total else None
    terms = []
    for lines in fluxes:
        per = []
        for low, high in lines:
            gain, both = low - high, low + high
            per.append((gain, -3.0 * both, 2.0 * gain))
        terms.append(per)
    out = []
    for i in range(3):
        for j in range(3):
            for l in range(3):
                v = values[mode(i, j, l)]
                f = factor[LAM[i] + LAM[j] + LAM[l]]
                v = v if f is None else v * f
                v = v + heats[i] * yz[3 * j + l]
                v = v + (terms[0][3 * j + l][i] + terms[1][3 * i + l][j]) + terms[2][3 * i + j][l]
                out.append(v)
    return out


def gauss_exp(offset, near, far):
    scaled = offset * jnp.where(offset >= 0.0, 1.0 / near, 1.0 / far)
    return jnp.exp(-3.0 * (scaled * scaled))


def place(m0, x, y, block):
    m0[pl.ds((x + 4) * 512 + slot(y), ROWS, stride=16), :] = block


def place_h(h0, row, y, blocks):
    lane = lane_iota(ROWS)
    rolled = [roll_lanes(b, (32 * n - 32 * y) % 128) if (n - y) % 4 else b for n, b in enumerate(blocks)]
    v = jnp.where(lane < 32, rolled[0], jnp.where(lane < 64, rolled[1], rolled[2]))
    h0[pl.ds(row, ROWS, stride=16), :] = jnp.where(lane < 96, v, 0.0)


def pair(ref, p, m):
    a = ref[pl.ds((4 + 2 * p) * 512 + 16 * m, 8), :]
    b = ref[pl.ds((5 + 2 * p) * 512 + 16 * m, 8), :]
    return jnp.where(row_iota(8) < 4, pltpu.roll(a, 6, axis=0), pltpu.roll(b, 2, axis=0))


LOW = [mode(i, j, l) for i in range(2) for j in range(2) for l in range(2)]


def line_modes(base, centre, near, far):
    return modal(*[gauss_exp(base + 0.5 * n - centre, near, far) for n in range(3)])


def pre_kernel(
    cols_ref, h_ref, xa_ref, xb_ref, own_in, cell_in,
    m0, h0, yz, yzh, xtab, xhtab, old, bmat, own_out,
    cell_ref, sems,
):
    gx, gy, gz = lax.axis_index("gx"), lax.axis_index("gy"), lax.axis_index("gz")
    even_x = upper_first("gx")
    fetch(((own_in, own_out), (cell_in, cell_ref)), sems)

    def clear(xi, _):
        for m in range(ROWS):
            m0[pl.ds(pl.multiple_of(xi * 512 + 16 * m, 16), 8), :] = jnp.zeros((8, 128), F32)
        return 0

    lax.fori_loop(1, 11, clear, 0)
    h0[...] = jnp.zeros((512, 128), F32)
    xhalo = functools.partial(xhalo_block, even_x, xa_ref, xb_ref)
    for c in range(16):
        place(m0, c // 4, c % 4, cols_ref[c * 32 : c * 32 + ROWS, :])
    for side in (0, 1):
        for y in range(4):
            place(m0, -1 if side == 0 else 4, y, xhalo(side, X1[y], ROWS))
            block = xhalo(side, X2[y], FAR)
            at = (2 if side == 0 else 9) * 512 + slot(y)
            m0[pl.ds(at, 9, stride=16), :] = block[0:9]
            m0[pl.ds(at + 18 * 16, 11, stride=16), :] = block[9:20]
    blocks = [xhalo(0, XH, ROWS), h_ref[0:ROWS, :], xhalo(1, XH, ROWS)]
    for y in range(4):
        place_h(h0, slot(y), y, blocks)

    lane16 = lane_iota(16)
    idx16 = lane16 % 8
    s16 = row_iota(16)
    ypos = (gy * PY + jnp.where(s16 < 12, s16 - 2, s16 - 18)).astype(F32)
    ymodes = line_modes(ypos, NY * 0.5, NY / 4.0, NY / 4.0)
    zpos = (gz * PZ + lane16).astype(F32)
    zmodes = line_modes(zpos, NZ * 0.75, NZ / 8.0, NZ / 8.0)
    zhpos = (gz * PZ + jnp.where(idx16 < 4, idx16 - 4, idx16 + 124)).astype(F32)
    zhmodes = line_modes(zhpos, NZ * 0.75, NZ / 8.0, NZ / 8.0)
    for j in range(3):
        for l in range(3):
            at = (3 * j + l) * 16
            yz[at : at + 16, :] = ymodes[j] * zmodes[l]
            yzh[at : at + 16, :] = ymodes[j] * zhmodes[l]
    for step in range(STEPS):
        centre = NX * 0.5 + step * NX / 16.0
        for t, v in enumerate(line_modes((gx * PX + s16 - 4).astype(F32), centre, NX / 8.0, NX / 4.0)):
            xtab[(3 * step + t) * 16 : (3 * step + t) * 16 + 16, :] = v
        for t, v in enumerate(line_modes((gx * PX + lane_iota(8) // 8 - 4).astype(F32), centre, NX / 8.0, NX / 4.0)):
            xhtab[(3 * step + t) * 8 : (3 * step + t) * 8 + 8, :] = v

    for g, m in enumerate(LOW):
        for p in range(2):
            old[16 * g + 8 * p : 16 * g + 8 * p + 8, :] = pair(m0, p, m)
    for c in range(16):
        cell = jnp.broadcast_to(cell_ref[c : c + 1, :], (CELLS, 128))
        hit = cell == row_iota(CELLS)
        bmat[:, 128 * c : 128 * c + 128] = jnp.where(hit, 1.0, 0.0).astype(jnp.bfloat16)


def main_kernel(
    m0_in, h0_in, yz, yzh, xtab, xhtab, old, bmat, xa_ref, xb_ref, ya_ref, yb_ref, h_ref, own_ref, live_ref,
    t_out, pay_out, m0, h0,
    m1, h1, cx, cy, czu, czd, ch, gs, q_ref, inc, amat, csum,
):
    del m0_in, h0_in
    even_y = upper_first("gy")
    lane8 = lane_iota(8)
    zeros8 = jnp.zeros((8, 128), F32)

    def yhalo(side, at, rows):
        a, b = ya_ref[at : at + rows, :], yb_ref[at : at + rows, :]
        return jnp.where(even_y, b, a) if side == 0 else jnp.where(even_y, a, b)

    for side in (0, 1):
        out = [-d if side == 0 else 3 + d for d in range(3)]
        for x in range(4):
            place(m0, x, out[1], yhalo(side, Y1[x], ROWS))
            block = yhalo(side, Y2[x], FAR)
            at = (x + 4) * 512 + slot(out[2])
            for i in range(3):
                for j in (0, 1):
                    row = 6 * i + 3 * j
                    m0[pl.ds(at + (9 * i + 6 * j) * 16, 3, stride=16), :] = block[row : row + 3]
            m0[pl.ds(at + 27 * 16, 2, stride=16), :] = block[18:20]
        for xside, at in NEAR:
            place(m0, -1 if xside == 0 else 4, out[1], yhalo(side, at, ROWS))
        for xside, xd, d, at in EDGE:
            block = yhalo(side, at, 4)
            to = ((-xd if xside == 0 else 3 + xd) + 4) * 512 + slot(out[d])
            m0[pl.ds(to, 3, stride=16), :] = block[0:3]
            m0[pl.ds(to + 27 * 16, 1), :] = block[3:4]
        beside = yhalo(side, YH[1], ROWS)
        blocks = [beside, yhalo(side, YH[0], ROWS), beside]
        for d in (1, 2):
            place_h(h0, slot(out[d]), out[d] % 4, blocks)

    idx8 = lane8 % 8
    kh = h0[27 * 16 : 27 * 16 + 8, :]
    last_row = row_iota(8) == 7
    gk_src = jnp.where(idx8 == 5, roll_lanes(kh, 2), kh)
    ch[0:8, :] = couple(kh, roll_lanes(kh, 120))
    ch[16:24, :] = jnp.where(last_row, 0.0, couple(kh, shift_rows(kh, True)))
    ch[32:40, :] = jnp.where((idx8 == 3) | (idx8 == 7), 0.0, couple(kh, roll_lanes(kh, 127)))
    ks = [m0[xi * 512 + 27 * 16 : xi * 512 + 27 * 16 + 8, :] for xi in range(1, 11)]
    for xi in range(1, 10):
        k, at = ks[xi - 1], slice(xi * 16, xi * 16 + 8)
        cx[at, :] = couple(k, ks[xi])
        if xi == 1:
            continue
        gk = roll_lanes(gk_src, 123 - xi * 8)
        cy[at, :] = jnp.where(last_row, 0.0, couple(k, shift_rows(k, True)))
        czu[at, :] = couple(k, jnp.where(lane8 == 127, gk, roll_lanes(k, 127)))
        czd[at, :] = couple(k, gk)

    def rows_of(ref, xi, n):
        return [ref[pl.ds(pl.multiple_of(xi * 512 + 16 * m, 8), n), :] for m in range(27)]

    def at_x(ref, xi, n):
        return ref[pl.ds(pl.multiple_of(xi * 16, 8), n), :]

    def table(ref, n):
        return [ref[16 * t : 16 * t + n, :] for t in range(9)]

    groups = [
        [(2, 10)],
        [(3, 9)],
        [(3, 9)],
        [(4, 6), (6, 8)],
    ]
    live = live_ref[...]

    def finish(ref, p):
        modes = [pair(ref, p, m) for m in range(27)]
        for n, v in enumerate(nodal_grid(modes)):
            t_out[n, 8 * p : 8 * p + 8, :] = v
        for g, m in enumerate(LOW):
            at = 16 * g + 8 * p
            inc[at : at + 8, :] = (modes[m] - old[at : at + 8, :]) * live

    src, dst, hsrc, hdst = m0, m1, h0, h1
    for step in range(STEPS):
        last = step == STEPS - 1
        hn = 8
        hv = [hsrc[16 * m : 16 * m + hn, :] for m in range(27)]
        lane_h = lane_iota(hn)
        idx_h = lane_h % 8
        hz = line_faces(hv, 1)
        for t, (low, high) in enumerate(hz):
            gs[16 * t : 16 * t + hn, :] = jnp.where(idx_h == 5, roll_lanes(high, 2), low)
        if not last:
            for t in range(9):
                q_ref[8 * t : 8 * t + 8, :] = zeros8

        n = 8
        for first, end in groups[step]:
            lane_n = lane_iota(n)

            def xflux(here, there, xi, n=n):
                c = at_x(cx, xi, n)
                return tuple(c * (a[1] - b[0]) for a, b in zip(line_faces(here, 9), line_faces(there, 9)))

            def body(xi, carry, n=n, src=src, dst=dst, step=step, last=last, lane_n=lane_n):
                left = carry
                values = rows_of(src, xi, n)
                following = rows_of(src, xi + 1, n)
                right = xflux(values, following, xi, n)
                kappa = DT * src_k(xi, n)
                heat = src_a(xi, n)
                xm = [xtab[pl.ds((3 * step + t) * 16 + xi, 1), :] for t in range(3)]
                heats = [heat * jnp.broadcast_to(v, (n, 128)) for v in xm]
                c = at_x(cy, xi, n)
                yf = []
                for low, high in line_faces(values, 3):
                    up = c * (high - shift_rows(low, True))
                    yf.append((shift_rows(up, False), up))
                cu, cd = at_x(czu, xi, n), at_x(czd, xi, n)
                zf = []
                shift = 123 - xi * 8
                mine = (lane8 == xi * 8 + 4) | (lane8 == xi * 8 + 5)
                for t, (low, high) in enumerate(line_faces(values, 1)):
                    g = roll_lanes(gs[16 * t : 16 * t + n, :], shift)
                    up = cu * (high - jnp.where(lane_n == 127, g, roll_lanes(low, 127)))
                    down = jnp.where(lane_n == 0, cd * (g - low), roll_lanes(up, 1))
                    zf.append((down, up))
                    if not last:
                        back = roll_lanes(jnp.where(lane8 == 127, up[0:8], down[0:8]), xi * 8 + 5)
                        q_ref[8 * t : 8 * t + 8, :] = jnp.where(mine, back, q_ref[8 * t : 8 * t + 8, :])
                out = advance(values, kappa, heats, table(yz, n), (list(zip(left, right)), yf, zf))
                for m, v in enumerate(out):
                    dst[pl.ds(pl.multiple_of(xi * 512 + 16 * m, 8), n), :] = v
                return right

            def src_k(xi, n):
                return m0[pl.ds(pl.multiple_of(xi * 512 + 27 * 16, 8), n), :]

            def src_a(xi, n):
                return m0[pl.ds(pl.multiple_of(xi * 512 + 28 * 16, 8), n), :]

            left = xflux(rows_of(src, first - 1, n), rows_of(src, first, n), first - 1, n)
            if end - first <= 8:
                for xi in range(first, end):
                    left = body(xi, left)
                if last:
                    finish(dst, first // 2 - 2)
            else:
                lax.fori_loop(0, (end - first) // 2, lambda t, c: body(first + 2 * t + 1, body(first + 2 * t, c)), left)

        if not last:
            n = 8
            inner = [v[0:8] for v in hv]
            idx_n = lane_iota(n) % 8
            xm = [xhtab[(3 * step + t) * 8 : (3 * step + t) * 8 + 8, :] for t in range(3)]
            heat = h0[28 * 16 : 28 * 16 + n, :]
            heats = [heat * wide(v, n) for v in xm]
            c = ch[0:n, :]
            xf = []
            for low, high in line_faces(inner, 9):
                up = c * (high - roll_lanes(low, 120))
                xf.append((roll_lanes(up, 8), up))
            c = ch[16 : 16 + n, :]
            yf = []
            for low, high in line_faces(inner, 3):
                up = c * (high - shift_rows(low, True))
                yf.append((shift_rows(up, False), up))
            c = ch[32 : 32 + n, :]
            zf = []
            for t, (low, high) in enumerate(line_faces(inner, 1)):
                up = c * (high - roll_lanes(low, 127))
                q = wide(q_ref[8 * t : 8 * t + 8, :], n)
                down = jnp.where(idx_n == 4, q, roll_lanes(up, 1))
                zf.append((down, jnp.where(idx_n == 3, roll_lanes(q, 126), up)))
            kappa = DT * h0[27 * 16 : 27 * 16 + n, :]
            out = advance(inner, kappa, heats, table(yzh, n), (xf, yf, zf))
            for m, v in enumerate(out):
                hdst[16 * m : 16 * m + n, :] = v
        src, dst, hsrc, hdst = dst, src, hdst, hsrc

    slots = (row_iota(16) + FIRST) % OWNERS
    for c in range(16):
        lanes = slice(128 * c, 128 * c + 128)
        v = inc[pl.ds(c, 8, stride=16), :]
        hi = v.astype(jnp.bfloat16).astype(F32)
        lo = v - hi
        owner = jnp.broadcast_to(own_ref[c : c + 1, :], (8, 128))
        picks = [owner == (o + FIRST) % OWNERS for o in range(OWNERS)]
        amat[0:128, lanes] = jnp.concatenate([jnp.where(k, hi, 0.0) for k in picks], axis=0).astype(jnp.bfloat16)
        amat[128:256, lanes] = jnp.concatenate([jnp.where(k, lo, 0.0) for k in picks], axis=0).astype(jnp.bfloat16)
        owner16 = jnp.broadcast_to(own_ref[c : c + 1, :], (16, 128))
        amat[256:272, lanes] = jnp.where(owner16 == slots, wide(live, 16), 0.0).astype(jnp.bfloat16)
    total = lax.dot_general(
        amat[...], bmat[...], (((1,), (1,)), ((), ())), preferred_element_type=F32
    )
    csum[0:128, :] = (total[0:128] + total[128:256])[:, 0:128]
    csum[128:256, :] = (total[0:128] + total[128:256])[:, 128:256]
    for h in range(2):
        for g in range(8):
            pay_out[pl.ds(2 * g + h, 16, stride=18), :] = csum[pl.ds(128 * h + g, 16, stride=8), :]
        pay_out[pl.ds(16 + h, 16, stride=18), :] = total[256:272, 128 * h : 128 * h + 128]


def gradient_table():
    spots = [0.5 - 0.5 / math.sqrt(3.0), 0.5 + 0.5 / math.sqrt(3.0)]
    out = np.zeros((3, 8, 8), np.float32)
    for node in range(8):
        corner = [node // 4, node // 2 % 2, node % 2]
        for point in range(8):
            place = [spots[point // 4], spots[point // 2 % 2], spots[point % 2]]
            values = [place[k] if corner[k] else 1.0 - place[k] for k in range(3)]
            slopes = [1.0 if corner[k] else -1.0 for k in range(3)]
            out[0, node, point] = slopes[0] * values[1] * values[2] / 8.0
            out[1, node, point] = values[0] * slopes[1] * values[2] / 8.0
            out[2, node, point] = values[0] * values[1] * slopes[2] / 8.0
    return out


def column(values):
    rows = row_iota(8)
    out = jnp.full((8, 128), float(values[7]), F32)
    for r in range(7):
        out = jnp.where(rows == r, float(values[r]), out)
    return out


def mechanics_kernel(
    got_ref, de_ref, st_ref, lim_ref, t_ref, stress_hbm, force_hbm, t_hbm, stress_out, force_out, sems, t_sem
):
    t_copy = pltpu.make_async_copy(t_ref, t_hbm, t_sem)
    t_copy.start()
    sums = got_ref[0:18, :]
    for s in range(1, OWNERS):
        sums = sums + got_ref[18 * s : 18 * s + 18, :]
    root = 1.0 / math.sqrt(3.0)
    rows = row_iota(8)
    signs = [jnp.where(rows // w % 2 == 0, -root, root) for w in (4, 2, 1)]
    table = gradient_table()
    cols = [[column(table[d, :, g]) for g in range(8)] for d in range(3)]
    for h in range(2):
        lanes = slice(128 * h, 128 * h + 128)
        inv = 1.0 / jnp.maximum(sums[16 + h : 17 + h], 1.0)

        def row(m):
            return jnp.broadcast_to(sums[2 * m + h : 2 * m + h + 1] * inv, (8, 128))

        z = [row(2 * n) + signs[2] * row(2 * n + 1) for n in range(4)]
        y = [z[2 * n] + signs[1] * z[2 * n + 1] for n in range(2)]
        strain = EXPANSION * (y[0] + signs[0] * y[1])
        normal = [de_ref[k, :, lanes] - strain for k in range(3)]
        volume = normal[0] + normal[1] + normal[2]
        trial = [st_ref[k, :, lanes] + LAME * volume + 2.0 * MU * normal[k] for k in range(3)]
        shear = [st_ref[k, :, lanes] + 2.0 * MU * de_ref[k, :, lanes] for k in range(3, 6)]
        pressure = (trial[0] + trial[1] + trial[2]) * (1.0 / 3.0)
        dev = [t - pressure for t in trial]
        squares = dev[0] * dev[0] + dev[1] * dev[1] + dev[2] * dev[2]
        squares = squares + 2.0 * (shear[0] * shear[0] + shear[1] * shear[1] + shear[2] * shear[2])
        equivalent = jnp.sqrt(1.5 * squares)
        limit = jnp.broadcast_to(lim_ref[0:1, lanes], (8, 128))
        plastic = jnp.maximum(equivalent - limit, 0.0) * (1.0 / (3.0 * MU + HARD))
        factor = 1.0 - (3.0 * MU) * plastic / jnp.maximum(equivalent, limit)
        stress = [pressure + factor * d for d in dev] + [factor * s for s in shear]
        for k in range(6):
            stress_out[k, :, lanes] = stress[k]
        index = [[0, 5, 4], [5, 1, 3], [4, 3, 2]]
        forces = [jnp.zeros((8, 128), F32)] * 3
        for g in range(8):
            at = [jnp.broadcast_to(s[g : g + 1], (8, 128)) for s in stress]
            for c in range(3):
                for d in range(3):
                    forces[c] = forces[c] + cols[d][g] * at[index[c][d]]
        for c in range(3):
            force_out[c, :, lanes] = forces[c]
    fetch(((stress_out, stress_hbm), (force_out, force_hbm)), sems)
    t_copy.wait()


def swap(first, second, axis, count):
    even = [(i, i ^ 1) for i in range(count)]
    odd = [(i, i + 1 if i % 2 else i - 1) for i in range(1, count - 1)]
    if axis == "gx":
        turns = lax.axis_size("gy")
        even, odd = (
            [(a * turns + t, b * turns + t) for t in range(turns) for a, b in (one, two)[t % 2]]
            for one, two in ((even, odd), (odd, even))
        )
        axis = ("gx", "gy")
    a = lax.ppermute(first, axis, even)
    b = lax.ppermute(second, axis, odd)
    return a, b


def program(temps, cond, absorb, layers, owner, cell, de, st, lim):
    vm = lambda n: pltpu.VMEM((n, 128), F32)
    sx, sy, sz = (lax.axis_size(a) for a in ("gx", "gy", "gz"))
    cols, zpay, live = call(
        prep_kernel,
        (vm(512), vm(32), vm(8)),
        (temps.reshape(27, 16, 128), cond.reshape(16, 128), absorb.reshape(16, 128), layers),
        scratch=[
            pltpu.VMEM((27, 16, 128), F32), vm(16), vm(16), pltpu.SemaphoreType.DMA((3,)),
        ],
        far=(0, 1, 2, 3),
    )
    za, zb = swap(zpay, zpay, "gz", sz)
    xf, xs, hown = call(xpay_kernel, (vm(XROWS), vm(XROWS), vm(32)), (cols, za, zb))
    xa, xb = swap(xf, xs, "gx", sx)
    yf, ys = call(ypay_kernel, (vm(YROWS), vm(YROWS)), (cols, xa, xb, hown))
    ya, yb = swap(yf, ys, "gy", sy)
    m0, h0, yz, yzh, xtab, xhtab, old, bmat, own = call(
        pre_kernel,
        (
            vm(6144), vm(512), vm(144), vm(144), vm(192), vm(96), vm(128),
            pltpu.VMEM((256, 2048), jnp.bfloat16), pltpu.VMEM((16, 128), jnp.int32),
        ),
        (cols, hown, xa, xb, owner.reshape(16, 128), cell.reshape(16, 128)),
        scratch=[pltpu.VMEM((16, 128), jnp.int32), pltpu.SemaphoreType.DMA((2,))],
        far=(4, 5),
    )
    t_new, pay, _, _ = call(
        main_kernel,
        (pltpu.VMEM((27, 16, 128), F32), vm(OWNERS * 18), vm(6144), vm(512)),
        (m0, h0, yz, yzh, xtab, xhtab, old, bmat, xa, xb, ya, yb, hown, own, live),
        scratch=[
            vm(6144), vm(512), vm(192), vm(192), vm(192), vm(192), vm(48), vm(144), vm(72), vm(128),
            pltpu.VMEM((272, 2048), jnp.bfloat16), vm(256),
        ],
        aliases={0: 2, 1: 3},
    )
    group = [(o + FIRST) % OWNERS for o in range(OWNERS)]
    got = lax.all_to_all(pay.reshape(OWNERS, 1, 2304), "gx", 0, 0, axis_index_groups=[group], tiled=True)
    stress, forces, t_new = call(
        mechanics_kernel,
        (pltpu.HBM((6, 8, 256), F32), pltpu.HBM((3, 8, 256), F32), pltpu.HBM((27, 16, 128), F32)),
        (got.reshape(OWNERS * 18, 128), de, st, lim.reshape(1, 256), t_new),
        scratch=[
            pltpu.VMEM((6, 8, 256), F32), pltpu.VMEM((3, 8, 256), F32),
            pltpu.SemaphoreType.DMA((2,)), pltpu.SemaphoreType.DMA,
        ],
    )
    return t_new.reshape(3, 3, 3, 4, 4, 128), stress, forces


def solution(mesh):
    cells = P(None, None, ("gx", "gy", "gz"))
    temps = P(None, None, None, "gx", "gy", "gz")
    block = P("gx", "gy", "gz")
    return jax.shard_map(
        program,
        mesh=mesh,
        in_specs=(
            temps, block, block, block, P("gx", "gy", "gz", None, None), P("gx", "gy", "gz", None),
            cells, cells, P(("gx", "gy", "gz")),
        ),
        out_specs=(temps, cells, cells),
        check_vma=False,
    )
```
